32 devices in a mesh: wide: 8 (over z, y), narrow: 4 (over x, core).
Axes of the slice: x: 2, y: 2, z: 4, core: 2. Of those that a mesh axis runs over, the one named last changes fastest.
Arguments:
- acoustic_features: bfloat16 [16384, 1024], P(('wide', 'narrow')), may hold values from -6 to 6
- utterance_durations: int32 [32, 8], P(('wide', 'narrow')), may hold values from 0 to 256, as said below
- perturbation_samples: bfloat16 [16384, 1024], P(('wide', 'narrow')), may hold values from -3 to 14, as said below
- annealing_level: float32 [1], replicated, may hold values from 0.5 to 2
- result_cotangent: bfloat16 [16384, 1024], P(('wide', 'narrow')), may hold values from -6 to 6
- quantized_cotangent: bfloat16 [16384, 1024], P(('wide', 'narrow')), may hold values from -6 to 6
- early_expanding_projector: bfloat16 [1024, 4096], P('narrow'), may hold values from -0.1875 to 0.1875
- early_contracting_projector: bfloat16 [4096, 1024], P('narrow'), may hold values from -0.25 to 0.25
- query_key_value_projector: bfloat16 [1024, 3072], P('narrow'), may hold values from -0.25 to 0.25
- heads_merging_projector: bfloat16 [1024, 1024], P('narrow'), may hold values from -0.5 to 0.5
- gated_channel_projector: bfloat16 [1024, 2048], P('narrow'), may hold values from -0.1875 to 0.1875
- closing_channel_projector: bfloat16 [1024, 1024], P('narrow'), may hold values from -0.25 to 0.25
- later_expanding_projector: bfloat16 [1024, 4096], P('narrow'), may hold values from -0.1875 to 0.1875
- later_contracting_projector: bfloat16 [4096, 1024], P('narrow'), may hold values from -0.25 to 0.25
- vocabulary_affinity_projector: bfloat16 [1024, 1024], P('narrow'), may hold values from -0.25 to 0.25
- vocabulary_vectors: bfloat16 [1024, 1024], P('narrow'), may hold values from -12 to 12
- normalizer_gains: bfloat16 [6, 1024], P(None, 'narrow'), may hold values from 0.25 to 1.75
- channelwise_kernel_weights: bfloat16 [5, 1024], P(None, 'narrow'), may hold values from -3 to 3
- normalizer_affine_rows: bfloat16 [2, 1024], P(None, 'narrow'), may hold values from 0.5 to 1.5
Outputs:
- output: bfloat16 [16384, 1024], P(('wide', 'narrow'))
- codes: bfloat16 [16384, 1024], P(('wide', 'narrow'))
- frames_gradient: bfloat16 [16384, 1024], P(('wide', 'narrow'))
- first_up_gradient: float32 [1024, 4096], P('narrow')
- first_down_gradient: float32 [4096, 1024], P('narrow')
- attention_in_gradient: float32 [1024, 3072], P('narrow')
- attention_out_gradient: float32 [1024, 1024], P('narrow')
- pointwise_in_gradient: float32 [1024, 2048], P('narrow')
- pointwise_out_gradient: float32 [1024, 1024], P('narrow')
- second_up_gradient: float32 [1024, 4096], P('narrow')
- second_down_gradient: float32 [4096, 1024], P('narrow')
- quantizer_in_gradient: float32 [1024, 1024], P('narrow')
- codebook_gradient: float32 [1024, 1024], P('narrow')
- norm_gains_gradient: float32 [6, 1024], P(None, 'narrow')
- depthwise_kernel_gradient: float32 [5, 1024], P(None, 'narrow')
- batch_affine_gradient: float32 [2, 1024], P(None, 'narrow')
The draws below stay inside these ranges and needn't reach their ends.
Inputs may be any that keep to these rules, and one draw needn't show every extreme that they name: `utterance_durations`: each entry is 0 (an empty slot) or 64, 128 or 256; in each row the nonempty slots come first and sum to at most 512; in every draw some row sums to exactly 512 and holds an utterance of 256. `perturbation_samples`: standard Gumbel samples.
All inputs are finite; a program needn't handle non-finite values.
Results may differ from the reference program's by a relative error of at most 0.024.
Values may be sent and summed in bfloat16 or wider, within the bound.
A program may use at most 320 MiB of HBM per device.

```python
import jax
import jax.numpy as jnp
from jax import lax

D = 1024
HEADS = 8
HEAD_DIM = 128
FF = 4096
KERNEL = 5
CODES = 1024
CODE_DIM = 1024
UNIT = 64
UNITS_DEV = 8
TOK_DEV = 512
HOLDERS = 32
FRAMES = 16384
N_WIDE = 8
N_NARROW = 4


def draw_utterance_durations(key, part):
    key_units, key_target, key_full = jax.random.split(key, 3)
    scores = jax.random.randint(key_units, (HOLDERS, UNITS_DEV), 0, 19)
    units = jnp.where(scores < 12, 1, jnp.where(scores < 16, 2, 4)).astype(jnp.int32)
    target = jax.random.randint(key_target, (HOLDERS, 1), UNITS_DEV // 2, UNITS_DEV + 1)
    reach = jnp.cumsum(units, axis=1)
    kept = jnp.where(reach <= target, units, 0).astype(jnp.int32)
    slot_index = jnp.arange(UNITS_DEV, dtype=jnp.int32)
    full_row = jnp.where(slot_index == 0, 4, jnp.where(slot_index <= UNITS_DEV - 4, 1, 0)).astype(jnp.int32)
    chosen = jax.random.randint(key_full, (), 0, HOLDERS)
    holder_index = jnp.arange(HOLDERS, dtype=jnp.int32)[:, None]
    result = jnp.where(holder_index == chosen, full_row[None, :], kept)
    return (result * UNIT).astype(jnp.int32)


def draw_perturbation_samples(key, part):
    uniform_draws = jax.random.uniform(key, (FRAMES, CODES), jnp.float32, 1e-06, 1.0 - 1e-06)
    return (-jnp.log(-jnp.log(uniform_draws))).astype(jnp.bfloat16)


def steps_of(own_key, shape, cuts, least, largest):
    def one(position, shards_of):
        draws = jax.random.uniform(jax.random.fold_in(jax.random.fold_in(own_key, 6), position), (shards_of,), jnp.float32, least / len(cuts), largest / len(cuts))
        return jnp.repeat(jnp.exp(draws), shape[position] // shards_of).reshape((-1,) + (1,) * (len(shape) - position - 1))

    loudness = one(*cuts[0])
    for cut in cuts[1:]:
        loudness = loudness * one(*cut)
    return loudness


def gaussian(rng, dims, scale, most, cuts=(), held_as=jnp.bfloat16):
    array = jax.random.normal(rng, dims, jnp.float32) * scale
    if len(cuts) > 0:
        array = steps_of(rng, dims, cuts, -0.22, 0.18) * array
    return jnp.clip(array, min=-most, max=most).astype(held_as)


def setup_inputs(seed: int = 0) -> dict:
    streams_of = jax.random.split(jax.random.key(seed), 20)
    return {
        "acoustic_features": gaussian(streams_of[0], (FRAMES, D), 1.0, 6.0, ((0, 32),)),
        "utterance_durations": draw_utterance_durations(jax.random.fold_in(streams_of[19], 71), 0),
        "perturbation_samples": draw_perturbation_samples(jax.random.fold_in(streams_of[19], 71), 0),
        "annealing_level": jnp.clip(jax.random.uniform(streams_of[3], (1,), jnp.float32, 0.5, 2.0), 0.5, 2.0),
        "result_cotangent": gaussian(streams_of[4], (FRAMES, D), 1.0, 6.0, ((0, 32),)),
        "quantized_cotangent": gaussian(streams_of[5], (FRAMES, CODE_DIM), 1.0, 6.0, ((0, 32),)),
        "early_expanding_projector": gaussian(streams_of[6], (D, FF), D ** -0.5, 0.1875, ((0, 4),)),
        "early_contracting_projector": gaussian(streams_of[7], (FF, D), (FF // 8) ** -0.5, 0.25, ((0, 4),)),
        "query_key_value_projector": gaussian(streams_of[8], (D, 3 * D), (D // 2) ** -0.5, 0.25, ((0, 4),)),
        "heads_merging_projector": gaussian(streams_of[9], (D, D), (D // 8) ** -0.5, 0.5, ((0, 4),)),
        "gated_channel_projector": gaussian(streams_of[10], (D, 2 * D), D ** -0.5, 0.1875, ((0, 4),)),
        "closing_channel_projector": gaussian(streams_of[11], (D, D), (D // 2) ** -0.5, 0.25, ((0, 4),)),
        "later_expanding_projector": gaussian(streams_of[12], (D, FF), D ** -0.5, 0.1875, ((0, 4),)),
        "later_contracting_projector": gaussian(streams_of[13], (FF, D), (FF // 8) ** -0.5, 0.25, ((0, 4),)),
        "vocabulary_affinity_projector": gaussian(streams_of[14], (D, CODES), (D // 2) ** -0.5, 0.25, ((0, 4),)),
        "vocabulary_vectors": gaussian(streams_of[15], (CODES, CODE_DIM), 2.0, 12.0, ((0, 4),)),
        "normalizer_gains": jnp.clip(1.0 + 0.15 * jax.random.normal(streams_of[16], (6, D), jnp.float32), 0.25, 1.75).astype(jnp.bfloat16),
        "channelwise_kernel_weights": gaussian(streams_of[17], (KERNEL, D), 0.5, 3.0, ((1, 4),)),
        "normalizer_affine_rows": jnp.clip(0.5 + 1.0 * jax.random.uniform(streams_of[18], (2, D), jnp.float32) ** steps_of(streams_of[18], (2, D), ((1, 4),), -0.2, 0.2), 0.5, 1.5).astype(jnp.bfloat16),
    }


@jax.custom_vjp
def low(v):
    return lax.optimization_barrier(v.astype(jnp.bfloat16)).astype(jnp.float32)

@jax.custom_vjp
def low_back(v):
    return v

def low_keep(v):
    return (low(v), None)

def low_pass(kept, grad):
    return (grad,)

def back_keep(v):
    return (v, None)

def back_low(kept, grad):
    return (low(grad),)
low.defvjp(low_keep, low_pass)
low_back.defvjp(back_keep, back_low)
EPSILON = 1e-05
NEGATIVE = -1e+30
EXACT = lax.Precision.HIGHEST

def matmul(left, right):
    return jnp.dot(left, right, precision=EXACT, preferred_element_type=jnp.float32)

def layer_norm(values, gain):
    centred = values - lax.optimization_barrier(jnp.mean(values, axis=-1, keepdims=True))
    return centred * lax.rsqrt(lax.optimization_barrier(jnp.mean(centred * centred, axis=-1, keepdims=True)) + EPSILON) * gain

def shift_rows(values, offset, fill):
    if offset == 0:
        return values
    padding = jnp.full((values.shape[0], abs(offset)) + values.shape[2:], fill, values.dtype)
    if offset > 0:
        return jnp.concatenate([values[:, offset:], padding], axis=1)
    return jnp.concatenate([padding, values[:, :offset]], axis=1)

def depthwise(values, kernel, segment):
    taps = kernel.shape[0]
    total = jnp.zeros_like(values)
    for tap_index in range(taps):
        offset = tap_index - taps // 2
        same_segment = (shift_rows(segment, offset, -1) == segment).astype(values.dtype)[..., None]
        total = total + kernel[tap_index] * shift_rows(values, offset, 0.0) * same_segment
    return total

def feed_forward(values, weight_in, weight_out, gain):
    entry = low(layer_norm(values, gain))
    before = low_back(matmul(entry, weight_in))
    return low_back(matmul(low(before * jax.nn.sigmoid(before)), weight_out))

def attend_holder(queries, keys, head_values, segment):
    factor = HEAD_DIM ** (-0.5)
    scores = low_back(jnp.einsum('ihd,jhd->hij', queries, keys, precision=EXACT) * factor)
    allowed = segment[:, None] == segment[None, :]
    scores = jnp.where(allowed[None], scores, NEGATIVE)
    weights = jax.nn.softmax(scores, axis=-1)
    return jnp.einsum('hij,jhd->ihd', low(weights), head_values, precision=EXACT)

def attend_one(pieces):
    return jax.checkpoint(attend_holder)(pieces[0], pieces[1], pieces[2], pieces[3])

def forward(inputs, segment, valid, noise_values, annealing_divisor, params):
    early_expanding_projector, early_contracting_projector, query_key_value_projector, heads_merging_projector, gated_channel_projector, closing_channel_projector, later_expanding_projector, later_contracting_projector, vocabulary_affinity_projector, vocabulary_vectors, normalizer_gains, channelwise_kernel_weights, normalizer_affine_rows = params
    holders, row_count, width = inputs.shape
    flat = inputs.reshape(holders * row_count, width)
    mask = valid.reshape(-1, 1)
    quantizer_entry = low(layer_norm(flat, normalizer_gains[0]))
    vocabulary_affinity = low_back(matmul(quantizer_entry, vocabulary_affinity_projector))
    code_probabilities = jax.nn.softmax((vocabulary_affinity + noise_values) / annealing_divisor, axis=-1)
    codes = matmul(low(code_probabilities), vocabulary_vectors)
    after_first = flat + 0.5 * feed_forward(flat, early_expanding_projector, early_contracting_projector, normalizer_gains[1])
    mixed = low(low_back(matmul(low(layer_norm(after_first, normalizer_gains[2])), query_key_value_projector)))
    shaped = mixed.reshape(holders, row_count, 3, HEADS, HEAD_DIM)
    heads_out = lax.map(attend_one, (shaped[:, :, 0], shaped[:, :, 1], shaped[:, :, 2], segment))
    heads_out = low(low_back(heads_out.reshape(holders * row_count, width)))
    after_attention = after_first + low_back(matmul(heads_out, heads_merging_projector))
    gates = low_back(matmul(low(layer_norm(after_attention, normalizer_gains[3])), gated_channel_projector))
    gated = gates[:, :width] * jax.nn.sigmoid(gates[:, width:])
    convolved = depthwise(gated.reshape(holders, row_count, width), channelwise_kernel_weights, segment).reshape(-1, width)
    count = jnp.sum(mask)
    mean = lax.optimization_barrier(jnp.sum(convolved * mask, axis=0)) / count
    centred = convolved - mean
    spread = lax.optimization_barrier(jnp.sum(centred * centred * mask, axis=0)) / count
    batch_out = centred * lax.rsqrt(spread + EPSILON) * normalizer_affine_rows[0] + normalizer_affine_rows[1]
    after_conv = after_attention + low_back(matmul(low(batch_out * jax.nn.sigmoid(batch_out)), closing_channel_projector))
    after_second = after_conv + 0.5 * feed_forward(after_conv, later_expanding_projector, later_contracting_projector, normalizer_gains[4])
    return (layer_norm(after_second, normalizer_gains[5]), codes)

def reference(acoustic_features, utterance_durations, perturbation_samples, annealing_level, result_cotangent, quantized_cotangent, early_expanding_projector, early_contracting_projector, query_key_value_projector, heads_merging_projector, gated_channel_projector, closing_channel_projector, later_expanding_projector, later_contracting_projector, vocabulary_affinity_projector, vocabulary_vectors, normalizer_gains, channelwise_kernel_weights, normalizer_affine_rows):
    holders = N_WIDE * N_NARROW
    positions = jnp.arange(TOK_DEV, dtype=jnp.int32)
    slot_ends = jnp.cumsum(utterance_durations, axis=1).astype(jnp.int32)
    segment = lax.optimization_barrier(jnp.sum((positions[None, :, None] >= slot_ends[:, None, :]).astype(jnp.int32), axis=2)).astype(jnp.int32)
    valid = (positions[None, :] < slot_ends[:, -1:]).astype(jnp.float32)
    inputs = acoustic_features.astype(jnp.float32).reshape(holders, TOK_DEV, D)
    params = tuple((weight.astype(jnp.float32) for weight in (early_expanding_projector, early_contracting_projector, query_key_value_projector, heads_merging_projector, gated_channel_projector, closing_channel_projector, later_expanding_projector, later_contracting_projector, vocabulary_affinity_projector, vocabulary_vectors, normalizer_gains, channelwise_kernel_weights, normalizer_affine_rows)))
    noise_values = perturbation_samples.astype(jnp.float32)
    annealing_divisor = annealing_level[0]

    def run(values, params_now):
        return forward(values, segment, valid, noise_values, annealing_divisor, params_now)
    (output, codes), pull = jax.vjp(run, inputs, params)
    mask = valid.reshape(-1, 1)
    adjoint_inputs, adjoint_params = pull((result_cotangent.astype(jnp.float32) * mask, quantized_cotangent.astype(jnp.float32) * mask))
    scaled = [entry / N_WIDE for entry in adjoint_params]
    return (output.astype(jnp.bfloat16), codes.astype(jnp.bfloat16), adjoint_inputs.reshape(-1, D).astype(jnp.bfloat16), scaled[0], scaled[1], scaled[2], scaled[3], scaled[4], scaled[5], scaled[6], scaled[7], scaled[8], scaled[9], scaled[10], scaled[11], scaled[12])
```

```python
import functools

import jax
import jax.numpy as jnp
from jax import lax
from jax.experimental import pallas as pl
from jax.experimental.pallas import tpu as pltpu
from jax.sharding import PartitionSpec as P

HEADS = 8
MESH = pl.DeviceIdType.MESH

EPSILON = 1e-05
NEGATIVE = -1e30


def flipped(index, bit):
    step = 1 << bit
    return index + step * (1 - 2 * ((index // step) % 2))


def bit_of(index, bit):
    return (index // (1 << bit)) % 2


def bits_of(size):
    return size.bit_length() - 1


def gather_kernel(count, direct, *refs):
    shards, wholes = refs[:count], refs[count : 2 * count]
    send, recv, own_in, own_out = refs[2 * count : 2 * count + 4]
    held = refs[2 * count + 4 :]
    me, wide = lax.axis_index("narrow"), lax.axis_index("wide")
    near, far = {"narrow": flipped(me, 0)}, {"narrow": flipped(me, 1)}
    across = flipped(me, 1)
    sides = ({"wide": flipped(wide, 0)}, {"wide": flipped(wide, 1)})
    side_bits = (bit_of(wide, 0), bit_of(wide, 1))
    barrier = pltpu.get_barrier_semaphore()
    for peer in (near, far) + sides:
        pl.semaphore_signal(barrier, inc=1, device_id=peer, device_id_type=MESH)
    pl.semaphore_wait(barrier, 4)
    started = []

    def start(k, slot, src, dst, peer):
        copy = pltpu.make_async_remote_copy(
            src_ref=src,
            dst_ref=dst,
            send_sem=send.at[k, slot],
            recv_sem=recv.at[k, slot],
            device_id=peer,
            device_id_type=MESH,
        )
        copy.start()
        started.append(copy)
        return copy

    def rows(k, block, first, size):
        begin = pl.multiple_of(block * shards[k].shape[0] + first, 16)
        return wholes[k].at[pl.ds(begin, size)]

    plan, crossing = [], []
    turn = 0
    for k in range(count):
        depth = shards[k].shape[0]
        if direct[k]:
            plan.append(None)
            crossing.append(start(k, 0, shards[k], rows(k, me, 0, depth), far))
        else:
            a, b = turn, 1 - turn
            turn = b
            quarter = depth // 4
            first = (side_bits[b] * 2 + side_bits[a]) * quarter
            plan.append((a, b, quarter, first))
            piece = shards[k].at[pl.ds(pl.multiple_of(first, 16), quarter)]
            crossing.append(start(k, 0, piece, rows(k, me, first, quarter), far))
    taken = [pltpu.make_async_copy(shards[k], held[k], own_in.at[k]) for k in range(count)]
    for copy in taken:
        copy.start()
    own = [
        start(k, 1, shards[k], rows(k, me, 0, shards[k].shape[0]), near) for k in range(count)
    ]
    placed, second, third, last = [], {}, {}, []
    for step in range(count + 2):
        k = step
        if k < count:
            crossing[k].wait_recv()
            depth = shards[k].shape[0]
            if plan[k] is None:
                block = rows(k, across, 0, depth)
                last.append(start(k, 2, block, block, near))
            else:
                a, b, quarter, first = plan[k]
                block = rows(k, across, first, quarter)
                second[k] = start(k, 2, block, block, sides[a])
            taken[k].wait()
            placed.append(
                pltpu.make_async_copy(held[k], rows(k, me, 0, depth), own_out.at[k])
            )
            placed[-1].start()
        k = step - 1
        if k in second:
            second[k].wait_recv()
            a, b, quarter, first = plan[k]
            block = rows(k, across, side_bits[b] * 2 * quarter, 2 * quarter)
            third[k] = start(k, 3, block, block, sides[b])
            last.append(start(k, 4, block, block, near))
        k = step - 2
        if k in third:
            third[k].wait_recv()
            a, b, quarter, first = plan[k]
            block = rows(k, across, (1 - side_bits[b]) * 2 * quarter, 2 * quarter)
            last.append(start(k, 5, block, block, near))
    for copy in own + last:
        copy.wait_recv()
    for copy in started:
        copy.wait_send()
    for copy in placed:
        copy.wait()


def gather_all(shards, direct):
    count = len(shards)
    parts = lax.axis_size("narrow")
    return pl.pallas_call(
        functools.partial(gather_kernel, count, direct),
        out_shape=[
            jax.ShapeDtypeStruct((shard.shape[0] * parts, shard.shape[1]), shard.dtype)
            for shard in shards
        ],
        in_specs=[pl.BlockSpec(memory_space=pl.ANY)] * count,
        out_specs=[pl.BlockSpec(memory_space=pl.ANY)] * count,
        scratch_shapes=[
            pltpu.SemaphoreType.DMA((count, 6)),
            pltpu.SemaphoreType.DMA((count, 6)),
            pltpu.SemaphoreType.DMA((count,)),
            pltpu.SemaphoreType.DMA((count,)),
        ]
        + [pltpu.VMEM(shard.shape, shard.dtype) for shard in shards],
        compiler_params=pltpu.CompilerParams(collective_id=0, has_side_effects=True),
    )(*shards)


def spread_kernel(across, within, sliced, mine_ref, all_ref, send, recv):
    total = across * within
    me = lax.axis_index("wide") * within + lax.axis_index("narrow")

    def peer_of(step):
        peer = lax.rem(me + step, total)
        return (peer // within, lax.rem(peer, within))

    barrier = pltpu.get_barrier_semaphore()

    def greet(step, carry):
        pl.semaphore_signal(barrier, inc=1, device_id=peer_of(step), device_id_type=MESH)
        return carry

    lax.fori_loop(1, total, greet, 0)
    pl.semaphore_wait(barrier, total - 1)

    def copy_of(step):
        return pltpu.make_async_remote_copy(
            src_ref=mine_ref.at[lax.rem(me + step, within) if sliced else 0],
            dst_ref=all_ref.at[me],
            send_sem=send.at[step],
            recv_sem=recv.at[step],
            device_id=peer_of(step),
            device_id_type=MESH,
        )

    def begin(step, carry):
        copy_of(step).start()
        return carry

    lax.fori_loop(1, total, begin, 0)
    all_ref[me] = mine_ref[lax.axis_index("narrow") if sliced else 0]

    def finish(step, carry):
        copy_of(step).wait()
        return carry

    lax.fori_loop(1, total, finish, 0)


def from_all(mine, identity, sliced=False):
    across, within = lax.axis_size("wide"), lax.axis_size("narrow")
    total = across * within
    rows, width = mine.shape
    pieces = within if sliced else 1
    split = jnp.transpose(mine.reshape(rows, pieces, width // pieces), (1, 0, 2))
    split = split.reshape(pieces, rows * width // pieces // 128, 128)
    everyone = pl.pallas_call(
        functools.partial(spread_kernel, across, within, sliced),
        out_shape=jax.ShapeDtypeStruct((total,) + split.shape[1:], split.dtype),
        in_specs=[pl.BlockSpec(memory_space=pltpu.VMEM)],
        out_specs=pl.BlockSpec(memory_space=pltpu.VMEM),
        scratch_shapes=[pltpu.SemaphoreType.DMA((total,)), pltpu.SemaphoreType.DMA((total,))],
        compiler_params=pltpu.CompilerParams(collective_id=identity, has_side_effects=True),
    )(split)
    return everyone.reshape(total, rows, width // pieces)


COLS = 512
ROWS = 256
LAGS = 10


def gradient_kernel(plan, depth, extra, scale, *refs):
    count = len(plan)
    lefts, rights, outs = refs[:count], refs[count : 2 * count], refs[2 * count : 3 * count]
    (
        left_buf,
        right_buf,
        near_send,
        near_recv,
        held,
        far_send,
        far_recv,
        kept,
        half_send,
        half_recv,
        half_kept,
        quarter_send,
        quarter_recv,
        quarter_kept,
        eighth_send,
        eighth_recv,
        eighth_kept,
        whole_send,
        whole_recv,
        back_eighth,
        back_eighth_recv,
        back_quarter,
        back_quarter_recv,
        back_half,
        back_half_recv,
        out_buf,
        fetch_sem,
        out_sem,
        sends,
        recvs,
    ) = refs[3 * count :]
    total = sum(units for _, units, _, _ in plan)
    me, wide = lax.axis_index("narrow"), lax.axis_index("wide")
    core, side = bit_of(me, 0), bit_of(me, 1)
    near, far = {"narrow": flipped(me, 0)}, {"narrow": flipped(me, 1)}
    bits = [bit_of(wide, i) for i in range(3)]
    peers = [near, far] + [{"wide": flipped(wide, i)} for i in range(3 + extra)]
    barrier = pltpu.get_barrier_semaphore()
    for peer in peers:
        pl.semaphore_signal(barrier, inc=1, device_id=peer, device_id_type=MESH)
    pl.semaphore_wait(barrier, len(peers))

    def order_of(unit):
        turn = lax.rem(unit, 2)
        first = bits[0] * (1 - turn) + bits[1] * turn
        second = bits[1] * (1 - turn) + bits[0] * turn
        near_step, far_step = 1 - 2 * bits[0], 2 * (1 - 2 * bits[1])
        first_peer = {"wide": wide + near_step * (1 - turn) + far_step * turn}
        second_peer = {"wide": wide + far_step * (1 - turn) + near_step * turn}
        return first, second, bits[2], first_peer, second_peer, {"wide": flipped(wide, 2)}

    def exchange(stage, unit, slots, source, target, peer):
        slot = lax.rem(unit, slots)
        return pltpu.make_async_remote_copy(
            src_ref=source.at[slot],
            dst_ref=target.at[slot],
            send_sem=sends.at[stage, slot],
            recv_sem=recvs.at[stage, slot],
            device_id=peer,
            device_id_type=MESH,
        )

    def fetches(i, unit, slot):
        first, _, width, per_row = plan[i]
        place = unit - first
        deep, col = place // per_row, lax.rem(place, per_row)
        copies = []
        for n in range(4):
            begin = pl.multiple_of(n * (width // 4) + deep * ROWS, ROWS)
            copies.append(
                pltpu.make_async_copy(
                    lefts[i].at[:, pl.ds(begin, ROWS)],
                    left_buf.at[slot, n],
                    fetch_sem.at[slot, n],
                )
            )
        begin = pl.multiple_of(col * COLS, COLS)
        copies.append(
            pltpu.make_async_copy(
                rights[i].at[:, pl.ds(begin, COLS)], right_buf.at[slot], fetch_sem.at[slot, 4]
            )
        )
        return copies

    def fetch(unit):
        for i, (first, units, _, _) in enumerate(plan):

            @pl.when((unit >= first) & (unit < first + units))
            def _(i=i):
                for copy in fetches(i, unit, lax.rem(unit, 2)):
                    copy.start()

    def placing(i, unit, slot):
        first, _, _, per_row = plan[i]
        place = unit - first
        deep, col = place // per_row, lax.rem(place, per_row)
        block = outs[i].at[
            pl.ds(pl.multiple_of(deep * ROWS, ROWS), ROWS),
            pl.ds(pl.multiple_of(col * COLS, COLS), COLS),
        ]
        return pltpu.make_async_copy(out_buf.at[slot], block, out_sem.at[slot])

    def by_rows(rows, body):
        def step(r, carry):
            body(pl.multiple_of(r * 32, 32))
            return carry

        if rows == 32:
            body(0)
        else:
            lax.fori_loop(0, rows // 32, step, 0)

    def added(first, first_slot, first_row, second, second_slot, second_row):
        return first[first_slot, pl.ds(first_row, 32), :].astype(jnp.float32) + second[
            second_slot, pl.ds(second_row, 32), :
        ].astype(jnp.float32)

    def stage_of(lag, tick, body):
        unit = tick - lag

        @pl.when((unit >= 0) & (unit < total))
        def _():
            body(unit)

    def split(unit, rows, bit, kept_in, arrived, slot, send_to, keep_in):
        half = rows // 2

        def body(r):
            theirs, mine = (1 - bit) * half + r, bit * half + r
            send_to[slot, pl.ds(r, 32), :] = added(
                kept_in, slot, theirs, arrived, slot, theirs
            ).astype(jnp.bfloat16)
            keep_in[slot, pl.ds(r, 32), :] = added(kept_in, slot, mine, arrived, slot, mine)

        by_rows(half, body)

    def joined(rows, bit, mine, arrived, slot, target, convert):
        half = rows // 2

        def body(r):
            target[slot, pl.ds(bit * half + r, 32), :] = convert(mine[slot, pl.ds(r, 32), :])
            target[slot, pl.ds((1 - bit) * half + r, 32), :] = convert(
                arrived[slot, pl.ds(r, 32), :]
            )

        by_rows(half, body)

    def finish(unit):
        first, _, _, first_peer, _, _ = order_of(unit)
        exchange(7, unit, 4, back_half, back_half_recv, first_peer).wait()
        slot = lax.rem(unit, 4)

        @pl.when(unit >= 4)
        def _():
            placing(0, unit * 0, slot).wait()

        joined(
            ROWS, first, back_half, back_half_recv, slot, out_buf,
            lambda v: v.astype(jnp.float32) * scale,
        )
        for i, (start, units, _, _) in enumerate(plan):

            @pl.when((unit >= start) & (unit < start + units))
            def _(i=i):
                placing(i, unit, slot).start()

    def double_last(unit):
        _, second, _, first_peer, second_peer, _ = order_of(unit)
        exchange(6, unit, 4, back_quarter, back_quarter_recv, second_peer).wait()
        joined(
            ROWS // 2, second, back_quarter, back_quarter_recv, lax.rem(unit, 4), back_half,
            lambda v: v,
        )
        exchange(7, unit, 4, back_half, back_half_recv, first_peer).start()

    def double_first(unit):
        _, _, third, _, second_peer, third_peer = order_of(unit)
        exchange(5, unit, 4, back_eighth, back_eighth_recv, third_peer).wait()
        joined(
            ROWS // 4, third, back_eighth, back_eighth_recv, lax.rem(unit, 4), back_quarter,
            lambda v: v,
        )
        exchange(6, unit, 4, back_quarter, back_quarter_recv, second_peer).start()

    def turn_back(unit):
        _, _, _, _, _, third_peer = order_of(unit)
        slot = lax.rem(unit, 4)
        exchange(4, unit, 4, eighth_send, eighth_recv, third_peer).wait()
        value = added(eighth_kept, slot, 0, eighth_recv, slot, 0)
        for bit in range(3, 3 + extra):
            whole_send[slot] = value.astype(jnp.bfloat16)
            copy = exchange(5 + bit, unit, 4, whole_send, whole_recv.at[bit - 3], {"wide": flipped(wide, bit)})
            copy.start()
            copy.wait()
            value = value + whole_recv[bit - 3, slot].astype(jnp.float32)
        back_eighth[slot] = value.astype(jnp.bfloat16)
        exchange(5, unit, 4, back_eighth, back_eighth_recv, third_peer).start()

    def halve_third(unit):
        _, _, third, _, second_peer, third_peer = order_of(unit)
        slot = lax.rem(unit, 4)
        exchange(3, unit, 4, quarter_send, quarter_recv, second_peer).wait()
        split(unit, ROWS // 4, third, quarter_kept, quarter_recv, slot, eighth_send, eighth_kept)
        exchange(4, unit, 4, eighth_send, eighth_recv, third_peer).start()

    def halve_second(unit):
        _, second, _, first_peer, second_peer, _ = order_of(unit)
        slot = lax.rem(unit, 4)
        exchange(2, unit, 4, half_send, half_recv, first_peer).wait()
        split(unit, ROWS // 2, second, half_kept, half_recv, slot, quarter_send, quarter_kept)
        exchange(3, unit, 4, quarter_send, quarter_recv, second_peer).start()

    def halve_first(unit):
        first, _, _, first_peer, _, _ = order_of(unit)
        slot = lax.rem(unit, 4)
        exchange(1, unit, 4, far_send, far_recv, far).wait()
        split(unit, ROWS, first, kept, far_recv, slot, half_send, half_kept)
        exchange(2, unit, 4, half_send, half_recv, first_peer).start()

    def cross(unit):
        slot, near_slot = lax.rem(unit, 4), lax.rem(unit, 2)
        exchange(0, unit, 2, near_send, near_recv, near).wait()

        def body(r):
            far_send[slot, pl.ds(r, 32), :] = (
                held[near_slot, 0, pl.ds(r, 32), :]
                + near_recv[near_slot, 0, pl.ds(r, 32), :].astype(jnp.float32)
            ).astype(jnp.bfloat16)
            kept[slot, pl.ds(r, 32), :] = held[near_slot, 1, pl.ds(r, 32), :] + near_recv[
                near_slot, 1, pl.ds(r, 32), :
            ].astype(jnp.float32)

        by_rows(ROWS, body)
        exchange(1, unit, 4, far_send, far_recv, far).start()

    def multiply(unit):
        slot = lax.rem(unit, 2)
        for copy in fetches(0, unit * 0, slot):
            copy.wait()

        @pl.when(unit + 1 < total)
        def _():
            fetch(unit + 1)

        def product(block, first):
            return lax.dot_general(
                left_buf[slot, block],
                right_buf[slot, :, pl.ds(first, 256)],
                (((0,), (0,)), ((), ())),
                preferred_element_type=jnp.float32,
            )

        for which in range(2):
            block = 2 * (side * which + (1 - side) * (1 - which)) + 1 - core
            for first in range(0, COLS, 256):
                near_send[slot, which, :, pl.ds(first, 256)] = product(block, first).astype(
                    jnp.bfloat16
                )
        exchange(0, unit, 2, near_send, near_recv, near).start()
        for which in range(2):
            block = 2 * (side * which + (1 - side) * (1 - which)) + core
            for first in range(0, COLS, 256):
                held[slot, which, :, pl.ds(first, 256)] = product(block, first)

    fetch(me * 0)

    def tick(step, carry):
        stage_of(9, step, finish)
        stage_of(8, step, double_last)
        stage_of(7, step, double_first)
        stage_of(6, step, turn_back)
        stage_of(5, step, halve_third)
        stage_of(4, step, halve_second)
        stage_of(3, step, halve_first)
        stage_of(1, step, cross)
        stage_of(0, step, multiply)
        return carry

    lax.fori_loop(0, total + LAGS - 1, tick, 0)
    for slot in range(4):
        placing(0, me * 0, slot).wait()


def gradients(pairs):
    parts, copies = lax.axis_size("narrow"), lax.axis_size("wide")
    extra = bits_of(copies) - 3
    plan, begun = [], 0
    for left, right in pairs:
        per_row = right.shape[1] // COLS
        units = per_row * (left.shape[1] // (parts * ROWS))
        plan.append((begun, units, left.shape[1], per_row))
        begun += units
    rows = pairs[0][0].shape[0]
    low, high = jnp.bfloat16, jnp.float32

    def pair_of(size, slots=4):
        return [pltpu.VMEM((slots, size, COLS), low)] * 2

    def trio_of(size):
        return pair_of(size) + [pltpu.VMEM((4, size, COLS), high)]

    scratch = (
        [
            pltpu.VMEM((2, 4, rows, ROWS), low),
            pltpu.VMEM((2, rows, COLS), low),
            pltpu.VMEM((2, 2, ROWS, COLS), low),
            pltpu.VMEM((2, 2, ROWS, COLS), low),
            pltpu.VMEM((2, 2, ROWS, COLS), high),
        ]
        + trio_of(ROWS)
        + trio_of(ROWS // 2)
        + trio_of(ROWS // 4)
        + trio_of(ROWS // 8)
        + [
            pltpu.VMEM((4, ROWS // 8, COLS), low),
            pltpu.VMEM((max(extra, 1), 4, ROWS // 8, COLS), low),
        ]
        + pair_of(ROWS // 8)
        + pair_of(ROWS // 4)
        + pair_of(ROWS // 2)
        + [
            pltpu.VMEM((4, ROWS, COLS), high),
            pltpu.SemaphoreType.DMA((2, 5)),
            pltpu.SemaphoreType.DMA((4,)),
            pltpu.SemaphoreType.DMA((8 + extra, 4)),
            pltpu.SemaphoreType.DMA((8 + extra, 4)),
        ]
    )
    count = len(pairs)
    return pl.pallas_call(
        functools.partial(gradient_kernel, tuple(plan), rows, extra, 1.0 / copies),
        out_shape=[
            jax.ShapeDtypeStruct((left.shape[1] // parts, right.shape[1]), high)
            for left, right in pairs
        ],
        in_specs=[pl.BlockSpec(memory_space=pl.ANY)] * (2 * count),
        out_specs=[pl.BlockSpec(memory_space=pl.ANY)] * count,
        scratch_shapes=scratch,
        compiler_params=pltpu.CompilerParams(collective_id=4, has_side_effects=True),
    )(*[left for left, _ in pairs], *[right for _, right in pairs])


def matmul(left, right):
    return jnp.dot(left, right, preferred_element_type=jnp.float32)


def across_rows(left, right):
    return lax.dot_general(
        left, right, (((0,), (0,)), ((), ())), preferred_element_type=jnp.float32
    )


def against(left, right):
    return lax.dot_general(
        left, right, (((1,), (1,)), ((), ())), preferred_element_type=jnp.float32
    )


def swish_slope(values):
    sigmoid = jax.nn.sigmoid(values)
    return sigmoid * (1.0 + values * (1.0 - sigmoid))


def layer_norm(values, gain):
    centred = values - jnp.mean(values, axis=-1, keepdims=True)
    scale = lax.rsqrt(jnp.mean(centred * centred, axis=-1, keepdims=True) + EPSILON)
    normed = centred * scale
    return (normed * gain, normed, scale)


def norm_back(adjoint_out, normed, scale, gain):
    adjoint_normed = adjoint_out * gain
    gain_sum = jnp.sum(adjoint_out * normed, axis=0)
    adjoint_in = scale * (
        adjoint_normed
        - jnp.mean(adjoint_normed, axis=-1, keepdims=True)
        - normed * jnp.mean(adjoint_normed * normed, axis=-1, keepdims=True)
    )
    return (adjoint_in, gain_sum)


def shift_rows(values, offset, fill):
    if offset == 0:
        return values
    padding = jnp.full((abs(offset),) + values.shape[1:], fill, values.dtype)
    if offset > 0:
        return jnp.concatenate([values[offset:], padding], axis=0)
    return jnp.concatenate([padding, values[:offset]], axis=0)


def depthwise(values, kernel, segment):
    taps = kernel.shape[0]
    total = jnp.zeros_like(values)
    for tap_index in range(taps):
        offset = tap_index - taps // 2
        same_segment = (shift_rows(segment, offset, -1) == segment).astype(jnp.float32)[:, None]
        total = total + kernel[tap_index] * shift_rows(values, offset, 0.0) * same_segment
    return total


def depthwise_back(adjoint, values, kernel, segment):
    taps = kernel.shape[0]
    adjoint_values = jnp.zeros_like(values)
    kernel_rows = []
    for tap_index in range(taps):
        offset = tap_index - taps // 2
        same_segment = (shift_rows(segment, offset, -1) == segment).astype(jnp.float32)[:, None]
        masked = adjoint * same_segment
        kernel_rows.append(jnp.sum(masked * shift_rows(values, offset, 0.0), axis=0))
        adjoint_values = adjoint_values + shift_rows(masked * kernel[tap_index], -offset, 0.0)
    return (adjoint_values, jnp.stack(kernel_rows))


def feed_forward(values, weight_in, weight_out, gain):
    normed, normal_hat, scale = layer_norm(values, gain)
    entry = normed.astype(jnp.bfloat16)
    before = matmul(entry, weight_in)
    active = (before * jax.nn.sigmoid(before)).astype(jnp.bfloat16)
    branch = matmul(active, weight_out)
    return (values + 0.5 * branch, (entry, normal_hat, scale, before, active))


def feed_back(adjoint, kept, weight_in, weight_out, gain):
    entry, normal_hat, scale, before, active = kept
    adjoint_branch = (0.5 * adjoint).astype(jnp.bfloat16)
    adjoint_before = (against(adjoint_branch, weight_out) * swish_slope(before)).astype(
        jnp.bfloat16
    )
    adjoint_values, gain_sum = norm_back(
        against(adjoint_before, weight_in), normal_hat, scale, gain
    )
    return (
        adjoint + adjoint_values,
        (entry, adjoint_before),
        (active, adjoint_branch),
        gain_sum,
    )


def masked_scores(query_block, segment_block, keys, segment, factor):
    scores = (
        jnp.einsum("ihd,jhd->hij", query_block, keys, preferred_element_type=jnp.float32) * factor
    )
    allowed = segment_block[:, None] == segment[None, :]
    return jnp.where(allowed[None], scores, NEGATIVE)


def attention_forward(values, weight_in, weight_out, gain, segment, heads):
    normed, normal_hat, scale = layer_norm(values, gain)
    entry = normed.astype(jnp.bfloat16)
    mixed = matmul(entry, weight_in).astype(jnp.bfloat16)
    row_count, width = values.shape
    head_dim = width // heads
    block = min(512, row_count)
    blocks = row_count // block
    queries = mixed[:, :width].reshape(blocks, block, heads, head_dim)
    keys = mixed[:, width : 2 * width].reshape(row_count, heads, head_dim)
    head_values = mixed[:, 2 * width :].reshape(row_count, heads, head_dim)
    segment_blocks = segment.reshape(blocks, block)
    factor = head_dim ** (-0.5)

    def attend(pieces):
        query_block, segment_block = pieces
        scores = masked_scores(query_block, segment_block, keys, segment, factor)
        top = jnp.max(scores, axis=-1, keepdims=True)
        exponent = jnp.exp(scores - top)
        total = jnp.sum(exponent, axis=-1, keepdims=True)
        weights = (exponent / total).astype(jnp.bfloat16)
        result = jnp.einsum(
            "hij,jhd->ihd", weights, head_values, preferred_element_type=jnp.float32
        )
        return (result.astype(jnp.bfloat16), (top + jnp.log(total))[..., 0])

    outputs, log_totals = lax.map(attend, (queries, segment_blocks))
    heads_out = outputs.reshape(row_count, width)
    branch = matmul(heads_out, weight_out)
    kept = (
        entry,
        normal_hat,
        scale,
        queries,
        keys,
        head_values,
        segment_blocks,
        log_totals,
        heads_out,
    )
    return (values + branch, kept)


def attention_back(adjoint, kept, weight_in, weight_out, gain, segment, heads):
    entry, normal_hat, scale, queries, keys, head_values, segment_blocks, log_totals, heads_out = (
        kept
    )
    row_count, width = adjoint.shape
    blocks = queries.shape[0]
    block = queries.shape[1]
    head_dim = width // heads
    factor = head_dim ** (-0.5)
    adjoint_branch = adjoint.astype(jnp.bfloat16)
    adjoint_heads = (
        against(adjoint_branch, weight_out)
        .astype(jnp.bfloat16)
        .reshape(blocks, block, heads, head_dim)
    )

    def step_back(carry, pieces):
        key_sum, value_sum = carry
        query_block, segment_block, log_block, adjoint_block = pieces
        scores = masked_scores(query_block, segment_block, keys, segment, factor)
        weights = jnp.exp(scores - log_block[..., None])
        value_sum = value_sum + jnp.einsum(
            "hij,ihd->jhd",
            weights.astype(jnp.bfloat16),
            adjoint_block,
            preferred_element_type=jnp.float32,
        )
        adjoint_weights = jnp.einsum(
            "ihd,jhd->hij", adjoint_block, head_values, preferred_element_type=jnp.float32
        )
        adjoint_scores = (
            weights * (adjoint_weights - jnp.sum(weights * adjoint_weights, axis=-1, keepdims=True))
        ).astype(jnp.bfloat16)
        query_adjoint = (
            jnp.einsum("hij,jhd->ihd", adjoint_scores, keys, preferred_element_type=jnp.float32)
            * factor
        )
        key_sum = (
            key_sum
            + jnp.einsum(
                "hij,ihd->jhd", adjoint_scores, query_block, preferred_element_type=jnp.float32
            )
            * factor
        )
        return ((key_sum, value_sum), query_adjoint)

    zeros = jnp.zeros((row_count, heads, head_dim), jnp.float32)
    sums, query_adjoints = lax.scan(
        step_back, (zeros, zeros), (queries, segment_blocks, log_totals, adjoint_heads)
    )
    adjoint_mixed = jnp.concatenate(
        [
            query_adjoints.reshape(row_count, width),
            sums[0].reshape(row_count, width),
            sums[1].reshape(row_count, width),
        ],
        axis=1,
    ).astype(jnp.bfloat16)
    adjoint_values, gain_sum = norm_back(against(adjoint_mixed, weight_in), normal_hat, scale, gain)
    return (
        adjoint + adjoint_values,
        (entry, adjoint_mixed),
        (heads_out, adjoint_branch),
        gain_sum,
    )


def convolution_forward(values, weight_in, weight_out, small, segment, valid):
    taps = small.shape[0] - 3
    normed, normal_hat, scale = layer_norm(values, small[0])
    entry = normed.astype(jnp.bfloat16)
    gates = matmul(entry, weight_in)
    width = values.shape[1]
    sigmoid_right = jax.nn.sigmoid(gates[:, width:])
    gated = gates[:, :width] * sigmoid_right
    convolved = depthwise(gated, small[1 : 1 + taps], segment)
    here = jnp.sum(valid)
    total_here = jnp.sum(convolved * valid, axis=0)
    off = (convolved - total_here / jnp.maximum(here, 1.0)) * valid
    mine = jnp.stack([jnp.full((width,), here), total_here, jnp.sum(off * off, axis=0)])
    everyone = from_all(mine, 1)
    counts, totals, squares = everyone[:, 0], everyone[:, 1], everyone[:, 2]
    count = jnp.sum(counts, axis=0)
    mean = jnp.sum(totals, axis=0) / count
    apart = totals / jnp.maximum(counts, 1.0) - mean
    spread = jnp.sum(squares + counts * apart * apart, axis=0) / count
    centred = convolved - mean
    inverse = lax.rsqrt(spread + EPSILON)
    batch_hat = centred * inverse
    batch_out = batch_hat * small[1 + taps] + small[2 + taps]
    active = (batch_out * jax.nn.sigmoid(batch_out)).astype(jnp.bfloat16)
    branch = matmul(active, weight_out)
    kept = (
        entry,
        normal_hat,
        scale,
        gates,
        sigmoid_right,
        gated,
        batch_hat,
        batch_out,
        active,
        inverse,
        count,
    )
    return (values + branch, kept)


def convolution_back(adjoint, kept, weight_in, weight_out, small, segment, valid):
    (
        entry,
        normal_hat,
        scale,
        gates,
        sigmoid_right,
        gated,
        batch_hat,
        batch_out,
        active,
        inverse,
        count,
    ) = kept
    taps = small.shape[0] - 3
    width = adjoint.shape[1]
    adjoint_branch = adjoint.astype(jnp.bfloat16)
    adjoint_batch = against(adjoint_branch, weight_out) * swish_slope(batch_out)
    shift_sum = jnp.sum(adjoint_batch, axis=0)
    batch_gain_sum = jnp.sum(adjoint_batch * batch_hat, axis=0)
    adjoint_hat = adjoint_batch * small[1 + taps]
    sums = jnp.sum(
        from_all(
            jnp.stack(
                [
                    jnp.sum(adjoint_hat * valid, axis=0),
                    jnp.sum(adjoint_hat * batch_hat * valid, axis=0),
                ]
            ),
            2,
        ),
        axis=0,
    )
    first_total, second_total = sums[0], sums[1]
    adjoint_conv = inverse * (
        adjoint_hat - valid * (first_total + batch_hat * second_total) / count
    )
    adjoint_gated, kernel_sum = depthwise_back(adjoint_conv, gated, small[1 : 1 + taps], segment)
    left_half = gates[:, :width]
    adjoint_gates = jnp.concatenate(
        [
            adjoint_gated * sigmoid_right,
            adjoint_gated * left_half * sigmoid_right * (1.0 - sigmoid_right),
        ],
        axis=1,
    ).astype(jnp.bfloat16)
    adjoint_values, gain_sum = norm_back(
        against(adjoint_gates, weight_in), normal_hat, scale, small[0]
    )
    small_sum = jnp.concatenate(
        [gain_sum[None], kernel_sum, batch_gain_sum[None], shift_sum[None]], axis=0
    )
    return (
        adjoint + adjoint_values,
        (entry, adjoint_gates),
        (active, adjoint_branch),
        small_sum,
    )


def per_device(
    acoustic_features,
    utterance_durations,
    perturbation_samples,
    annealing_level,
    result_cotangent,
    quantized_cotangent,
    early_expanding_projector,
    early_contracting_projector,
    query_key_value_projector,
    heads_merging_projector,
    gated_channel_projector,
    closing_channel_projector,
    later_expanding_projector,
    later_contracting_projector,
    vocabulary_affinity_projector,
    vocabulary_vectors,
    normalizer_gains,
    channelwise_kernel_weights,
    normalizer_affine_rows,
):
    row_count = acoustic_features.shape[0]
    positions = lax.broadcasted_iota(jnp.int32, (row_count, 1), 0)
    slot_ends = jnp.cumsum(utterance_durations[0])
    segment = jnp.sum((positions >= slot_ends[None, :]).astype(jnp.int32), axis=1)
    valid = (positions < slot_ends[-1]).astype(jnp.float32)
    inputs = acoustic_features.astype(jnp.float32)
    taps = channelwise_kernel_weights.shape[0]
    gain_rows = normalizer_gains.shape[0]
    small = jnp.concatenate(
        [normalizer_gains, channelwise_kernel_weights, normalizer_affine_rows], axis=0
    )
    small_rows = small.shape[0]
    padding = -small_rows % 16
    small = jnp.pad(small, ((0, padding), (0, 0)))
    parts = lax.axis_size("narrow")
    order = (
        heads_merging_projector,
        gated_channel_projector,
        query_key_value_projector,
        early_expanding_projector,
        early_contracting_projector,
        later_expanding_projector,
        later_contracting_projector,
        closing_channel_projector,
        vocabulary_affinity_projector,
        vocabulary_vectors,
        small,
    )
    (
        attention_out,
        pointwise_in,
        attention_in,
        first_up,
        first_down,
        second_up,
        second_down,
        pointwise_out,
        quantizer_in,
        codebook,
        small_blocks,
    ) = gather_all(order, (False,) * 7 + (True,) * 4)
    small_whole = (
        jnp.transpose(small_blocks.reshape(parts, small_rows + padding, -1), (1, 0, 2))
        .reshape(small_rows + padding, -1)
        .astype(jnp.float32)
    )
    gains = small_whole[:gain_rows]
    conv_small = jnp.concatenate([gains[3:4], small_whole[gain_rows:small_rows]], axis=0)

    quantizer_normed, quantizer_hat, quantizer_scale = layer_norm(inputs, gains[0])
    quantizer_entry = quantizer_normed.astype(jnp.bfloat16)
    vocabulary_affinity = matmul(quantizer_entry, quantizer_in)
    code_probabilities = jax.nn.softmax(
        (vocabulary_affinity + perturbation_samples.astype(jnp.float32)) / annealing_level[0],
        axis=-1,
    )
    chances_low = code_probabilities.astype(jnp.bfloat16)
    codes = matmul(chances_low, codebook).astype(jnp.bfloat16)
    adjoint_codes = quantized_cotangent * valid.astype(jnp.bfloat16)
    adjoint_chances = against(adjoint_codes, codebook)
    adjoint_logits = (
        code_probabilities
        * (adjoint_chances - jnp.sum(code_probabilities * adjoint_chances, axis=-1, keepdims=True))
        / annealing_level[0]
    ).astype(jnp.bfloat16)
    adjoint_inputs, quantizer_gain_sum = norm_back(
        against(adjoint_logits, quantizer_in), quantizer_hat, quantizer_scale, gains[0]
    )

    after_first, first_kept = feed_forward(inputs, first_up, first_down, gains[1])
    after_attention, attend_kept = attention_forward(
        after_first, attention_in, attention_out, gains[2], segment, HEADS
    )
    after_conv, conv_kept = convolution_forward(
        after_attention, pointwise_in, pointwise_out, conv_small, segment, valid
    )
    after_second, second_kept = feed_forward(after_conv, second_up, second_down, gains[4])
    final_out, final_hat, final_scale = layer_norm(after_second, gains[5])
    output = final_out.astype(jnp.bfloat16)

    adjoint_output = result_cotangent.astype(jnp.float32) * valid
    adjoint, final_gain_sum = norm_back(adjoint_output, final_hat, final_scale, gains[5])
    adjoint, second_up_pair, second_down_pair, second_gain_sum = feed_back(
        adjoint, second_kept, second_up, second_down, gains[4]
    )
    adjoint, pointwise_in_pair, pointwise_out_pair, conv_small_sum = convolution_back(
        adjoint, conv_kept, pointwise_in, pointwise_out, conv_small, segment, valid
    )
    adjoint, attention_in_pair, attention_out_pair, attend_gain_sum = attention_back(
        adjoint, attend_kept, attention_in, attention_out, gains[2], segment, HEADS
    )
    adjoint, first_up_pair, first_down_pair, first_gain_sum = feed_back(
        adjoint, first_kept, first_up, first_down, gains[1]
    )
    (
        first_up_gradient,
        first_down_gradient,
        attention_in_gradient,
        attention_out_gradient,
        pointwise_in_gradient,
        pointwise_out_gradient,
        second_up_gradient,
        second_down_gradient,
        quantizer_in_gradient,
        codebook_gradient,
    ) = gradients(
        (
            first_up_pair,
            first_down_pair,
            attention_in_pair,
            attention_out_pair,
            pointwise_in_pair,
            pointwise_out_pair,
            second_up_pair,
            second_down_pair,
            (quantizer_entry, adjoint_logits),
            (chances_low, adjoint_codes),
        )
    )
    frames_gradient = (adjoint + adjoint_inputs).astype(jnp.bfloat16)
    small_sums = jnp.concatenate(
        [
            quantizer_gain_sum[None],
            first_gain_sum[None],
            attend_gain_sum[None],
            conv_small_sum[:1],
            second_gain_sum[None],
            final_gain_sum[None],
            conv_small_sum[1:],
        ],
        axis=0,
    )
    small_sums = jnp.pad(small_sums, ((0, padding), (0, 0)))
    small_gradient = jnp.sum(from_all(small_sums, 3, sliced=True), axis=0) / float(
        lax.axis_size("wide")
    )
    norm_gains_gradient = small_gradient[:gain_rows]
    depthwise_kernel_gradient = small_gradient[gain_rows : gain_rows + taps]
    batch_affine_gradient = small_gradient[gain_rows + taps : small_rows]
    return (
        output,
        codes,
        frames_gradient,
        first_up_gradient,
        first_down_gradient,
        attention_in_gradient,
        attention_out_gradient,
        pointwise_in_gradient,
        pointwise_out_gradient,
        second_up_gradient,
        second_down_gradient,
        quantizer_in_gradient,
        codebook_gradient,
        norm_gains_gradient,
        depthwise_kernel_gradient,
        batch_affine_gradient,
    )


def solution(mesh):
    in_specs = (
        P(("wide", "narrow"), None),
        P(("wide", "narrow"), None),
        P(("wide", "narrow"), None),
        P(),
        P(("wide", "narrow"), None),
        P(("wide", "narrow"), None),
        P("narrow", None),
        P("narrow", None),
        P("narrow", None),
        P("narrow", None),
        P("narrow", None),
        P("narrow", None),
        P("narrow", None),
        P("narrow", None),
        P("narrow", None),
        P("narrow", None),
        P(None, "narrow"),
        P(None, "narrow"),
        P(None, "narrow"),
    )
    out_specs = (
        P(("wide", "narrow"), None),
        P(("wide", "narrow"), None),
        P(("wide", "narrow"), None),
        P("narrow", None),
        P("narrow", None),
        P("narrow", None),
        P("narrow", None),
        P("narrow", None),
        P("narrow", None),
        P("narrow", None),
        P("narrow", None),
        P("narrow", None),
        P("narrow", None),
        P(None, "narrow"),
        P(None, "narrow"),
        P(None, "narrow"),
    )
    return jax.shard_map(
        per_device, mesh=mesh, in_specs=in_specs, out_specs=out_specs, check_vma=False
    )
```

```python
import functools

import jax
import jax.numpy as jnp
from jax import lax
from jax.experimental import pallas as pl
from jax.experimental.pallas import tpu as pltpu
from jax.sharding import PartitionSpec as P

HEADS = 8
MESH = pl.DeviceIdType.MESH

EPSILON = 1e-05
NEGATIVE = -1e30


def flipped(index, bit):
    step = 1 << bit
    return index + step * (1 - 2 * ((index // step) % 2))


def bit_of(index, bit):
    return (index // (1 << bit)) % 2


def bits_of(size):
    return size.bit_length() - 1


LAG = 2


def gather_kernel(plan, *refs):
    count = (len(refs) - 4) // 3
    shards, wholes = refs[:count], refs[count : 2 * count]
    send, recv, own_in, own_out = refs[2 * count : 2 * count + 4]
    held = refs[2 * count + 4 :]
    me, wide = lax.axis_index("narrow"), lax.axis_index("wide")
    near, far = {"narrow": flipped(me, 0)}, {"narrow": flipped(me, 1)}
    across = flipped(me, 1)
    sides = ({"wide": flipped(wide, 0)}, {"wide": flipped(wide, 1)})
    side_bits = (bit_of(wide, 0), bit_of(wide, 1))
    barrier = pltpu.get_barrier_semaphore()
    for peer in (near, far) + sides:
        pl.semaphore_signal(barrier, inc=1, device_id=peer, device_id_type=MESH)
    pl.semaphore_wait(barrier, 4)
    started = []

    def start(chunk, slot, src, dst, peer):
        copy = pltpu.make_async_remote_copy(
            src_ref=src,
            dst_ref=dst,
            send_sem=send.at[chunk, slot],
            recv_sem=recv.at[chunk, slot],
            device_id=peer,
            device_id_type=MESH,
        )
        copy.start()
        started.append(copy)
        return copy

    def rows(k, block, first, size):
        begin = pl.multiple_of(block * shards[k].shape[0] + first, 16)
        return wholes[k].at[pl.ds(begin, size)]

    crossing, routes = [], []
    turn = 0
    for chunk, (k, begin, size, direct) in enumerate(plan):
        if direct:
            routes.append(None)
            piece = shards[k].at[pl.ds(begin, size)]
            crossing.append(start(chunk, 0, piece, rows(k, me, begin, size), far))
        else:
            a, b = turn, 1 - turn
            turn = b
            quarter = size // 4
            first = begin + (side_bits[b] * 2 + side_bits[a]) * quarter
            routes.append((a, b, quarter, first))
            piece = shards[k].at[pl.ds(pl.multiple_of(first, 16), quarter)]
            crossing.append(start(chunk, 0, piece, rows(k, me, first, quarter), far))
    taken = [pltpu.make_async_copy(shards[k], held[k], own_in.at[k]) for k in range(count)]
    for copy in taken:
        copy.start()
    own = [
        start(len(plan) + k, 0, shards[k], rows(k, me, 0, shards[k].shape[0]), near)
        for k in range(count)
    ]
    placed, second, third, last = [], {}, {}, []
    for step in range(len(plan) + 2 * LAG):
        if step < count:
            taken[step].wait()
            depth = shards[step].shape[0]
            placed.append(
                pltpu.make_async_copy(held[step], rows(step, me, 0, depth), own_out.at[step])
            )
            placed[-1].start()
        chunk = step - 2 * LAG
        if chunk in third:
            third[chunk].wait_recv()
            k, begin, size, _ = plan[chunk]
            a, b, quarter, first = routes[chunk]
            block = rows(k, across, begin + (1 - side_bits[b]) * 2 * quarter, 2 * quarter)
            last.append(start(chunk, 5, block, block, near))
        chunk = step - LAG
        if chunk in second:
            second[chunk].wait_recv()
            k, begin, size, _ = plan[chunk]
            a, b, quarter, first = routes[chunk]
            block = rows(k, across, begin + side_bits[b] * 2 * quarter, 2 * quarter)
            third[chunk] = start(chunk, 3, block, block, sides[b])
            last.append(start(chunk, 4, block, block, near))
        chunk = step
        if chunk < len(plan):
            crossing[chunk].wait_recv()
            k, begin, size, direct = plan[chunk]
            if direct:
                block = rows(k, across, begin, size)
                last.append(start(chunk, 2, block, block, near))
            else:
                a, b, quarter, first = routes[chunk]
                block = rows(k, across, first, quarter)
                second[chunk] = start(chunk, 2, block, block, sides[a])
    for copy in own + last:
        copy.wait_recv()
    for copy in started:
        copy.wait_send()
    for copy in placed:
        copy.wait()


def chunks_of(shards, pieces):
    plan = []
    for k, (shard, cuts) in enumerate(zip(shards, pieces)):
        size = shard.shape[0] // max(cuts, 1)
        plan += [(k, i * size, size, cuts == 0) for i in range(max(cuts, 1))]
    return tuple(plan)


def gather_all(shards, plan):
    count = len(shards)
    parts = lax.axis_size("narrow")
    return pl.pallas_call(
        functools.partial(gather_kernel, plan),
        out_shape=[
            jax.ShapeDtypeStruct((shard.shape[0] * parts, shard.shape[1]), shard.dtype)
            for shard in shards
        ],
        in_specs=[pl.BlockSpec(memory_space=pl.ANY)] * count,
        out_specs=[pl.BlockSpec(memory_space=pl.ANY)] * count,
        scratch_shapes=[
            pltpu.SemaphoreType.DMA((len(plan) + count, 6)),
            pltpu.SemaphoreType.DMA((len(plan) + count, 6)),
            pltpu.SemaphoreType.DMA((count,)),
            pltpu.SemaphoreType.DMA((count,)),
        ]
        + [pltpu.VMEM(shard.shape, shard.dtype) for shard in shards],
        compiler_params=pltpu.CompilerParams(collective_id=0, has_side_effects=True),
    )(*shards)


def spread_kernel(across, within, mine_ref, all_ref, send, recv):
    total = across * within
    me = lax.axis_index("wide") * within + lax.axis_index("narrow")

    def peer_of(step):
        peer = lax.rem(me + step, total)
        return (peer // within, lax.rem(peer, within))

    barrier = pltpu.get_barrier_semaphore()

    def greet(step, carry):
        pl.semaphore_signal(barrier, inc=1, device_id=peer_of(step), device_id_type=MESH)
        return carry

    lax.fori_loop(1, total, greet, 0)
    pl.semaphore_wait(barrier, total - 1)

    def copy_of(step):
        return pltpu.make_async_remote_copy(
            src_ref=mine_ref,
            dst_ref=all_ref.at[me],
            send_sem=send.at[step],
            recv_sem=recv.at[step],
            device_id=peer_of(step),
            device_id_type=MESH,
        )

    def begin(step, carry):
        copy_of(step).start()
        return carry

    lax.fori_loop(1, total, begin, 0)
    all_ref[me] = mine_ref[...]

    def finish(step, carry):
        copy_of(step).wait()
        return carry

    lax.fori_loop(1, total, finish, 0)


def columns_split(small, pieces):
    rows, width = small.shape
    split = jnp.transpose(small.reshape(rows, pieces, width // pieces), (1, 0, 2))
    return split.reshape(pieces, rows * width // pieces // 128, 128)


def from_all(mine, identity):
    across, within = lax.axis_size("wide"), lax.axis_size("narrow")
    total = across * within
    flat = columns_split(mine, 1)[0]
    everyone = pl.pallas_call(
        functools.partial(spread_kernel, across, within),
        out_shape=jax.ShapeDtypeStruct((total,) + flat.shape, flat.dtype),
        in_specs=[pl.BlockSpec(memory_space=pltpu.VMEM)],
        out_specs=pl.BlockSpec(memory_space=pltpu.VMEM),
        scratch_shapes=[pltpu.SemaphoreType.DMA((total,)), pltpu.SemaphoreType.DMA((total,))],
        compiler_params=pltpu.CompilerParams(collective_id=identity, has_side_effects=True),
    )(flat)
    return everyone.reshape((total,) + mine.shape)


COLS = 256
ROWS = 256
LAGS = 16


def gradient_kernel(plan, extra, across, within, *refs):
    count = len(plan)
    lefts, rights = refs[:count], refs[count : 2 * count]
    small, outs, smalls = refs[2 * count], refs[2 * count + 1 : 3 * count + 1], refs[3 * count + 1]
    (
        left_buf,
        right_buf,
        near_send,
        near_recv,
        held,
        far_send,
        far_recv,
        kept,
        half_send,
        half_recv,
        half_kept,
        quarter_send,
        quarter_recv,
        quarter_kept,
        eighth_send,
        eighth_recv,
        eighth_kept,
        whole_send,
        whole_recv,
        back_eighth,
        back_eighth_recv,
        back_quarter,
        back_quarter_recv,
        back_half,
        back_half_recv,
        out_buf,
        fetch_sem,
        out_sem,
        sends,
        recvs,
        small_send,
        small_recv,
    ) = refs[3 * count + 2 :]
    total = sum(units for _, units, _, _ in plan)
    me, wide = lax.axis_index("narrow"), lax.axis_index("wide")
    core, side = bit_of(me, 0), bit_of(me, 1)
    near, far = {"narrow": flipped(me, 0)}, {"narrow": flipped(me, 1)}
    bits = [bit_of(wide, i) for i in range(3)]
    devices = across * within
    place = wide * within + me

    def peer_of(step):
        peer = lax.rem(place + step, devices)
        return (peer // within, lax.rem(peer, within))

    barrier = pltpu.get_barrier_semaphore()

    def greet(step, carry):
        pl.semaphore_signal(barrier, inc=1, device_id=peer_of(step), device_id_type=MESH)
        return carry

    lax.fori_loop(1, devices, greet, 0)
    pl.semaphore_wait(barrier, devices - 1)

    def small_copy(step):
        return pltpu.make_async_remote_copy(
            src_ref=small.at[lax.rem(place + step, within)],
            dst_ref=smalls.at[place],
            send_sem=small_send.at[step],
            recv_sem=small_recv.at[step],
            device_id=peer_of(step),
            device_id_type=MESH,
        )

    def begin(step, carry):
        small_copy(step).start()
        return carry

    def end(step, carry):
        small_copy(step).wait()
        return carry

    def order_of(unit):
        turn = lax.rem(unit, 2)
        first = bits[0] * (1 - turn) + bits[1] * turn
        second = bits[1] * (1 - turn) + bits[0] * turn
        near_step, far_step = 1 - 2 * bits[0], 2 * (1 - 2 * bits[1])
        first_peer = {"wide": wide + near_step * (1 - turn) + far_step * turn}
        second_peer = {"wide": wide + far_step * (1 - turn) + near_step * turn}
        return first, second, bits[2], first_peer, second_peer, {"wide": flipped(wide, 2)}

    def exchange(stage, unit, slots, source, target, peer):
        slot = lax.rem(unit, slots)
        return pltpu.make_async_remote_copy(
            src_ref=source.at[slot],
            dst_ref=target.at[slot],
            send_sem=sends.at[stage, slot],
            recv_sem=recvs.at[stage, slot],
            device_id=peer,
            device_id_type=MESH,
        )

    def fetches(i, unit, slot):
        first, _, width, per_row = plan[i]
        place = unit - first
        deep, col = place // per_row, lax.rem(place, per_row)
        copies = []
        for n in range(4):
            begin = pl.multiple_of(n * (width // 4) + deep * ROWS, ROWS)
            copies.append(
                pltpu.make_async_copy(
                    lefts[i].at[:, pl.ds(begin, ROWS)],
                    left_buf.at[slot, n],
                    fetch_sem.at[slot, n],
                )
            )
        begin = pl.multiple_of(col * COLS, COLS)
        copies.append(
            pltpu.make_async_copy(
                rights[i].at[:, pl.ds(begin, COLS)], right_buf.at[slot], fetch_sem.at[slot, 4]
            )
        )
        return copies

    def fetch(unit):
        for i, (first, units, _, _) in enumerate(plan):

            @pl.when((unit >= first) & (unit < first + units))
            def _(i=i):
                for copy in fetches(i, unit, lax.rem(unit, 2)):
                    copy.start()

    def placing(i, unit, slot):
        first, _, _, per_row = plan[i]
        place = unit - first
        deep, col = place // per_row, lax.rem(place, per_row)
        block = outs[i].at[
            pl.ds(pl.multiple_of(deep * ROWS, ROWS), ROWS),
            pl.ds(pl.multiple_of(col * COLS, COLS), COLS),
        ]
        return pltpu.make_async_copy(out_buf.at[slot], block, out_sem.at[slot])

    def by_rows(rows, body):
        def step(r, carry):
            body(pl.multiple_of(r * 32, 32))
            return carry

        if rows == 32:
            body(0)
        else:
            lax.fori_loop(0, rows // 32, step, 0)

    def added(first, first_slot, first_row, second, second_slot, second_row):
        return first[first_slot, pl.ds(first_row, 32), :].astype(jnp.float32) + second[
            second_slot, pl.ds(second_row, 32), :
        ].astype(jnp.float32)

    def stage_of(lag, tick, body):
        unit = tick - lag

        @pl.when((unit >= 0) & (unit < total))
        def _():
            body(unit)

    def split(unit, rows, bit, kept_in, arrived, slot, send_to, keep_in):
        half = rows // 2

        def body(r):
            theirs, mine = (1 - bit) * half + r, bit * half + r
            send_to[slot, pl.ds(r, 32), :] = added(
                kept_in, slot, theirs, arrived, slot, theirs
            ).astype(jnp.bfloat16)
            keep_in[slot, pl.ds(r, 32), :] = added(kept_in, slot, mine, arrived, slot, mine)

        by_rows(half, body)

    def joined(rows, bit, mine, arrived, slot, target):
        half = rows // 2

        def body(r):
            target[slot, pl.ds(bit * half + r, 32), :] = mine[slot, pl.ds(r, 32), :]
            target[slot, pl.ds((1 - bit) * half + r, 32), :] = arrived[slot, pl.ds(r, 32), :]

        by_rows(half, body)

    def finish(unit):
        first, _, _, first_peer, _, _ = order_of(unit)
        exchange(7, unit, 4, back_half, back_half_recv, first_peer).wait()
        slot = lax.rem(unit, 4)

        @pl.when(unit >= 4)
        def _():
            placing(0, unit * 0, slot).wait()

        joined(
            ROWS, first, back_half, back_half_recv, slot, out_buf,
        )
        for i, (start, units, _, _) in enumerate(plan):

            @pl.when((unit >= start) & (unit < start + units))
            def _(i=i):
                placing(i, unit, slot).start()

    def double_last(unit):
        _, second, _, first_peer, second_peer, _ = order_of(unit)
        exchange(6, unit, 4, back_quarter, back_quarter_recv, second_peer).wait()
        joined(
            ROWS // 2, second, back_quarter, back_quarter_recv, lax.rem(unit, 4), back_half,
        )
        exchange(7, unit, 4, back_half, back_half_recv, first_peer).start()

    def double_first(unit):
        _, _, third, _, second_peer, third_peer = order_of(unit)
        exchange(5, unit, 4, back_eighth, back_eighth_recv, third_peer).wait()
        joined(
            ROWS // 4, third, back_eighth, back_eighth_recv, lax.rem(unit, 4), back_quarter,
        )
        exchange(6, unit, 4, back_quarter, back_quarter_recv, second_peer).start()

    def turn_back(unit):
        _, _, _, _, _, third_peer = order_of(unit)
        slot = lax.rem(unit, 4)
        exchange(4, unit, 4, eighth_send, eighth_recv, third_peer).wait()
        value = added(eighth_kept, slot, 0, eighth_recv, slot, 0)
        for bit in range(3, 3 + extra):
            whole_send[slot] = value.astype(jnp.bfloat16)
            copy = exchange(5 + bit, unit, 4, whole_send, whole_recv.at[bit - 3], {"wide": flipped(wide, bit)})
            copy.start()
            copy.wait()
            value = value + whole_recv[bit - 3, slot].astype(jnp.float32)
        back_eighth[slot] = value.astype(jnp.bfloat16)
        exchange(5, unit, 4, back_eighth, back_eighth_recv, third_peer).start()

    def halve_third(unit):
        _, _, third, _, second_peer, third_peer = order_of(unit)
        slot = lax.rem(unit, 4)
        exchange(3, unit, 4, quarter_send, quarter_recv, second_peer).wait()
        split(unit, ROWS // 4, third, quarter_kept, quarter_recv, slot, eighth_send, eighth_kept)
        exchange(4, unit, 4, eighth_send, eighth_recv, third_peer).start()

    def halve_second(unit):
        _, second, _, first_peer, second_peer, _ = order_of(unit)
        slot = lax.rem(unit, 4)
        exchange(2, unit, 4, half_send, half_recv, first_peer).wait()
        split(unit, ROWS // 2, second, half_kept, half_recv, slot, quarter_send, quarter_kept)
        exchange(3, unit, 4, quarter_send, quarter_recv, second_peer).start()

    def halve_first(unit):
        first, _, _, first_peer, _, _ = order_of(unit)
        slot = lax.rem(unit, 4)
        exchange(1, unit, 4, far_send, far_recv, far).wait()
        split(unit, ROWS, first, kept, far_recv, slot, half_send, half_kept)
        exchange(2, unit, 4, half_send, half_recv, first_peer).start()

    def cross(unit):
        slot, near_slot = lax.rem(unit, 4), lax.rem(unit, 2)
        exchange(0, unit, 2, near_send, near_recv, near).wait()

        def body(r):
            far_send[slot, pl.ds(r, 32), :] = (
                held[near_slot, 0, pl.ds(r, 32), :]
                + near_recv[near_slot, 0, pl.ds(r, 32), :].astype(jnp.float32)
            ).astype(jnp.bfloat16)
            kept[slot, pl.ds(r, 32), :] = held[near_slot, 1, pl.ds(r, 32), :] + near_recv[
                near_slot, 1, pl.ds(r, 32), :
            ].astype(jnp.float32)

        by_rows(ROWS, body)
        exchange(1, unit, 4, far_send, far_recv, far).start()

    def multiply(unit):
        slot = lax.rem(unit, 2)
        for copy in fetches(0, unit * 0, slot):
            copy.wait()

        @pl.when(unit + 1 < total)
        def _():
            fetch(unit + 1)

        def product(block, first):
            return lax.dot_general(
                left_buf[slot, block],
                right_buf[slot, :, pl.ds(first, 256)],
                (((0,), (0,)), ((), ())),
                preferred_element_type=jnp.float32,
            )

        for which in range(2):
            block = 2 * (side * which + (1 - side) * (1 - which)) + 1 - core
            for first in range(0, COLS, 256):
                near_send[slot, which, :, pl.ds(first, 256)] = product(block, first).astype(
                    jnp.bfloat16
                )
        exchange(0, unit, 2, near_send, near_recv, near).start()
        for which in range(2):
            block = 2 * (side * which + (1 - side) * (1 - which)) + core
            for first in range(0, COLS, 256):
                held[slot, which, :, pl.ds(first, 256)] = product(block, first)

    fetch(me * 0)
    lax.fori_loop(1, devices, begin, 0)
    smalls[place] = small[me]

    def tick(step, carry):
        stage_of(15, step, finish)
        stage_of(13, step, double_last)
        stage_of(11, step, double_first)
        stage_of(9, step, turn_back)
        stage_of(7, step, halve_third)
        stage_of(5, step, halve_second)
        stage_of(3, step, halve_first)
        stage_of(1, step, cross)
        stage_of(0, step, multiply)
        return carry

    lax.fori_loop(0, total + LAGS - 1, tick, 0)
    for slot in range(4):
        placing(0, me * 0, slot).wait()
    lax.fori_loop(1, devices, end, 0)


def gradients(pairs, small):
    parts, copies = lax.axis_size("narrow"), lax.axis_size("wide")
    extra = bits_of(copies) - 3
    plan, begun = [], 0
    for left, right in pairs:
        per_row = right.shape[1] // COLS
        units = per_row * (left.shape[1] // (parts * ROWS))
        plan.append((begun, units, left.shape[1], per_row))
        begun += units
    rows = pairs[0][0].shape[0]
    low, high = jnp.bfloat16, jnp.float32

    def pair_of(size, slots=4):
        return [pltpu.VMEM((slots, size, COLS), low)] * 2

    def trio_of(size):
        return pair_of(size) + [pltpu.VMEM((4, size, COLS), high)]

    scratch = (
        [
            pltpu.VMEM((2, 4, rows, ROWS), low),
            pltpu.VMEM((2, rows, COLS), low),
            pltpu.VMEM((2, 2, ROWS, COLS), low),
            pltpu.VMEM((2, 2, ROWS, COLS), low),
            pltpu.VMEM((2, 2, ROWS, COLS), high),
        ]
        + trio_of(ROWS)
        + trio_of(ROWS // 2)
        + trio_of(ROWS // 4)
        + trio_of(ROWS // 8)
        + [
            pltpu.VMEM((4, ROWS // 8, COLS), low),
            pltpu.VMEM((max(extra, 1), 4, ROWS // 8, COLS), low),
        ]
        + pair_of(ROWS // 8)
        + pair_of(ROWS // 4)
        + pair_of(ROWS // 2)
        + [
            pltpu.VMEM((4, ROWS, COLS), low),
            pltpu.SemaphoreType.DMA((2, 5)),
            pltpu.SemaphoreType.DMA((4,)),
            pltpu.SemaphoreType.DMA((8 + extra, 4)),
            pltpu.SemaphoreType.DMA((8 + extra, 4)),
            pltpu.SemaphoreType.DMA((copies * parts,)),
            pltpu.SemaphoreType.DMA((copies * parts,)),
        ]
    )
    count = len(pairs)
    split = columns_split(small, parts)
    results = pl.pallas_call(
        functools.partial(gradient_kernel, tuple(plan), extra, copies, parts),
        out_shape=[
            jax.ShapeDtypeStruct((left.shape[1] // parts, right.shape[1]), low)
            for left, right in pairs
        ]
        + [jax.ShapeDtypeStruct((copies * parts,) + split.shape[1:], high)],
        in_specs=[pl.BlockSpec(memory_space=pl.ANY)] * (2 * count)
        + [pl.BlockSpec(memory_space=pltpu.VMEM)],
        out_specs=[pl.BlockSpec(memory_space=pl.ANY)] * count
        + [pl.BlockSpec(memory_space=pltpu.VMEM)],
        scratch_shapes=scratch,
        compiler_params=pltpu.CompilerParams(collective_id=4, has_side_effects=True),
    )(*[left for left, _ in pairs], *[right for _, right in pairs], split)
    everyone = results[-1].reshape(copies * parts, small.shape[0], -1)
    return tuple(whole.astype(high) / float(copies) for whole in results[:-1]) + (everyone,)


def matmul(left, right):
    return jnp.dot(left, right, preferred_element_type=jnp.float32)


def across_rows(left, right):
    return lax.dot_general(
        left, right, (((0,), (0,)), ((), ())), preferred_element_type=jnp.float32
    )


def against(left, right):
    return lax.dot_general(
        left, right, (((1,), (1,)), ((), ())), preferred_element_type=jnp.float32
    )


def swish_slope(values):
    sigmoid = jax.nn.sigmoid(values)
    return sigmoid * (1.0 + values * (1.0 - sigmoid))


def layer_norm(values, gain):
    centred = values - jnp.mean(values, axis=-1, keepdims=True)
    scale = lax.rsqrt(jnp.mean(centred * centred, axis=-1, keepdims=True) + EPSILON)
    normed = centred * scale
    return (normed * gain, normed, scale)


def norm_back(adjoint_out, normed, scale, gain):
    adjoint_normed = adjoint_out * gain
    gain_sum = jnp.sum(adjoint_out * normed, axis=0)
    adjoint_in = scale * (
        adjoint_normed
        - jnp.mean(adjoint_normed, axis=-1, keepdims=True)
        - normed * jnp.mean(adjoint_normed * normed, axis=-1, keepdims=True)
    )
    return (adjoint_in, gain_sum)


def shift_rows(values, offset, fill):
    if offset == 0:
        return values
    padding = jnp.full((abs(offset),) + values.shape[1:], fill, values.dtype)
    if offset > 0:
        return jnp.concatenate([values[offset:], padding], axis=0)
    return jnp.concatenate([padding, values[:offset]], axis=0)


def depthwise(values, kernel, segment):
    taps = kernel.shape[0]
    total = jnp.zeros_like(values)
    for tap_index in range(taps):
        offset = tap_index - taps // 2
        same_segment = (shift_rows(segment, offset, -1) == segment).astype(jnp.float32)[:, None]
        total = total + kernel[tap_index] * shift_rows(values, offset, 0.0) * same_segment
    return total


def depthwise_back(adjoint, values, kernel, segment):
    taps = kernel.shape[0]
    adjoint_values = jnp.zeros_like(values)
    kernel_rows = []
    for tap_index in range(taps):
        offset = tap_index - taps // 2
        same_segment = (shift_rows(segment, offset, -1) == segment).astype(jnp.float32)[:, None]
        masked = adjoint * same_segment
        kernel_rows.append(jnp.sum(masked * shift_rows(values, offset, 0.0), axis=0))
        adjoint_values = adjoint_values + shift_rows(masked * kernel[tap_index], -offset, 0.0)
    return (adjoint_values, jnp.stack(kernel_rows))


def feed_forward(values, weight_in, weight_out, gain):
    normed, normal_hat, scale = layer_norm(values, gain)
    entry = normed.astype(jnp.bfloat16)
    before = matmul(entry, weight_in)
    active = (before * jax.nn.sigmoid(before)).astype(jnp.bfloat16)
    branch = matmul(active, weight_out)
    return (values + 0.5 * branch, (entry, normal_hat, scale, before, active))


def feed_back(adjoint, kept, weight_in, weight_out, gain):
    entry, normal_hat, scale, before, active = kept
    adjoint_branch = (0.5 * adjoint).astype(jnp.bfloat16)
    adjoint_before = (against(adjoint_branch, weight_out) * swish_slope(before)).astype(
        jnp.bfloat16
    )
    adjoint_values, gain_sum = norm_back(
        against(adjoint_before, weight_in), normal_hat, scale, gain
    )
    return (
        adjoint + adjoint_values,
        (entry, adjoint_before),
        (active, adjoint_branch),
        gain_sum,
    )


def masked_scores(query_block, segment_block, keys, segment, factor):
    scores = (
        jnp.einsum("ihd,jhd->hij", query_block, keys, preferred_element_type=jnp.float32) * factor
    )
    allowed = segment_block[:, None] == segment[None, :]
    return jnp.where(allowed[None], scores, NEGATIVE)


def attention_forward(values, weight_in, weight_out, gain, segment, heads):
    normed, normal_hat, scale = layer_norm(values, gain)
    entry = normed.astype(jnp.bfloat16)
    mixed = matmul(entry, weight_in).astype(jnp.bfloat16)
    row_count, width = values.shape
    head_dim = width // heads
    block = min(512, row_count)
    blocks = row_count // block
    queries = mixed[:, :width].reshape(blocks, block, heads, head_dim)
    keys = mixed[:, width : 2 * width].reshape(row_count, heads, head_dim)
    head_values = mixed[:, 2 * width :].reshape(row_count, heads, head_dim)
    segment_blocks = segment.reshape(blocks, block)
    factor = head_dim ** (-0.5)

    def attend(pieces):
        query_block, segment_block = pieces
        scores = masked_scores(query_block, segment_block, keys, segment, factor)
        top = jnp.max(scores, axis=-1, keepdims=True)
        exponent = jnp.exp(scores - top)
        total = jnp.sum(exponent, axis=-1, keepdims=True)
        weights = (exponent / total).astype(jnp.bfloat16)
        result = jnp.einsum(
            "hij,jhd->ihd", weights, head_values, preferred_element_type=jnp.float32
        )
        return (result.astype(jnp.bfloat16), (top + jnp.log(total))[..., 0])

    outputs, log_totals = lax.map(attend, (queries, segment_blocks))
    heads_out = outputs.reshape(row_count, width)
    branch = matmul(heads_out, weight_out)
    kept = (
        entry,
        normal_hat,
        scale,
        queries,
        keys,
        head_values,
        segment_blocks,
        log_totals,
        heads_out,
    )
    return (values + branch, kept)


def attention_back(adjoint, kept, weight_in, weight_out, gain, segment, heads):
    entry, normal_hat, scale, queries, keys, head_values, segment_blocks, log_totals, heads_out = (
        kept
    )
    row_count, width = adjoint.shape
    blocks = queries.shape[0]
    block = queries.shape[1]
    head_dim = width // heads
    factor = head_dim ** (-0.5)
    adjoint_branch = adjoint.astype(jnp.bfloat16)
    adjoint_heads = (
        against(adjoint_branch, weight_out)
        .astype(jnp.bfloat16)
        .reshape(blocks, block, heads, head_dim)
    )

    def step_back(carry, pieces):
        key_sum, value_sum = carry
        query_block, segment_block, log_block, adjoint_block = pieces
        scores = masked_scores(query_block, segment_block, keys, segment, factor)
        weights = jnp.exp(scores - log_block[..., None])
        value_sum = value_sum + jnp.einsum(
            "hij,ihd->jhd",
            weights.astype(jnp.bfloat16),
            adjoint_block,
            preferred_element_type=jnp.float32,
        )
        adjoint_weights = jnp.einsum(
            "ihd,jhd->hij", adjoint_block, head_values, preferred_element_type=jnp.float32
        )
        adjoint_scores = (
            weights * (adjoint_weights - jnp.sum(weights * adjoint_weights, axis=-1, keepdims=True))
        ).astype(jnp.bfloat16)
        query_adjoint = (
            jnp.einsum("hij,jhd->ihd", adjoint_scores, keys, preferred_element_type=jnp.float32)
            * factor
        )
        key_sum = (
            key_sum
            + jnp.einsum(
                "hij,ihd->jhd", adjoint_scores, query_block, preferred_element_type=jnp.float32
            )
            * factor
        )
        return ((key_sum, value_sum), query_adjoint)

    zeros = jnp.zeros((row_count, heads, head_dim), jnp.float32)
    sums, query_adjoints = lax.scan(
        step_back, (zeros, zeros), (queries, segment_blocks, log_totals, adjoint_heads)
    )
    adjoint_mixed = jnp.concatenate(
        [
            query_adjoints.reshape(row_count, width),
            sums[0].reshape(row_count, width),
            sums[1].reshape(row_count, width),
        ],
        axis=1,
    ).astype(jnp.bfloat16)
    adjoint_values, gain_sum = norm_back(against(adjoint_mixed, weight_in), normal_hat, scale, gain)
    return (
        adjoint + adjoint_values,
        (entry, adjoint_mixed),
        (heads_out, adjoint_branch),
        gain_sum,
    )


def convolution_forward(values, weight_in, weight_out, small, segment, valid):
    taps = small.shape[0] - 3
    normed, normal_hat, scale = layer_norm(values, small[0])
    entry = normed.astype(jnp.bfloat16)
    gates = matmul(entry, weight_in)
    width = values.shape[1]
    sigmoid_right = jax.nn.sigmoid(gates[:, width:])
    gated = gates[:, :width] * sigmoid_right
    convolved = depthwise(gated, small[1 : 1 + taps], segment)
    here = jnp.sum(valid)
    total_here = jnp.sum(convolved * valid, axis=0)
    off = (convolved - total_here / jnp.maximum(here, 1.0)) * valid
    mine = jnp.stack([jnp.full((width,), here), total_here, jnp.sum(off * off, axis=0)])
    everyone = from_all(mine, 1)
    counts, totals, squares = everyone[:, 0], everyone[:, 1], everyone[:, 2]
    count = jnp.sum(counts, axis=0)
    mean = jnp.sum(totals, axis=0) / count
    apart = totals / jnp.maximum(counts, 1.0) - mean
    spread = jnp.sum(squares + counts * apart * apart, axis=0) / count
    centred = convolved - mean
    inverse = lax.rsqrt(spread + EPSILON)
    batch_hat = centred * inverse
    batch_out = batch_hat * small[1 + taps] + small[2 + taps]
    active = (batch_out * jax.nn.sigmoid(batch_out)).astype(jnp.bfloat16)
    branch = matmul(active, weight_out)
    kept = (
        entry,
        normal_hat,
        scale,
        gates,
        sigmoid_right,
        gated,
        batch_hat,
        batch_out,
        active,
        inverse,
        count,
    )
    return (values + branch, kept)


def convolution_back(adjoint, kept, weight_in, weight_out, small, segment, valid):
    (
        entry,
        normal_hat,
        scale,
        gates,
        sigmoid_right,
        gated,
        batch_hat,
        batch_out,
        active,
        inverse,
        count,
    ) = kept
    taps = small.shape[0] - 3
    width = adjoint.shape[1]
    adjoint_branch = adjoint.astype(jnp.bfloat16)
    adjoint_batch = against(adjoint_branch, weight_out) * swish_slope(batch_out)
    shift_sum = jnp.sum(adjoint_batch, axis=0)
    batch_gain_sum = jnp.sum(adjoint_batch * batch_hat, axis=0)
    adjoint_hat = adjoint_batch * small[1 + taps]
    sums = jnp.sum(
        from_all(
            jnp.stack(
                [
                    jnp.sum(adjoint_hat * valid, axis=0),
                    jnp.sum(adjoint_hat * batch_hat * valid, axis=0),
                ]
            ),
            2,
        ),
        axis=0,
    )
    first_total, second_total = sums[0], sums[1]
    adjoint_conv = inverse * (
        adjoint_hat - valid * (first_total + batch_hat * second_total) / count
    )
    adjoint_gated, kernel_sum = depthwise_back(adjoint_conv, gated, small[1 : 1 + taps], segment)
    left_half = gates[:, :width]
    adjoint_gates = jnp.concatenate(
        [
            adjoint_gated * sigmoid_right,
            adjoint_gated * left_half * sigmoid_right * (1.0 - sigmoid_right),
        ],
        axis=1,
    ).astype(jnp.bfloat16)
    adjoint_values, gain_sum = norm_back(
        against(adjoint_gates, weight_in), normal_hat, scale, small[0]
    )
    small_sum = jnp.concatenate(
        [gain_sum[None], kernel_sum, batch_gain_sum[None], shift_sum[None]], axis=0
    )
    return (
        adjoint + adjoint_values,
        (entry, adjoint_gates),
        (active, adjoint_branch),
        small_sum,
    )


def per_device(
    acoustic_features,
    utterance_durations,
    perturbation_samples,
    annealing_level,
    result_cotangent,
    quantized_cotangent,
    early_expanding_projector,
    early_contracting_projector,
    query_key_value_projector,
    heads_merging_projector,
    gated_channel_projector,
    closing_channel_projector,
    later_expanding_projector,
    later_contracting_projector,
    vocabulary_affinity_projector,
    vocabulary_vectors,
    normalizer_gains,
    channelwise_kernel_weights,
    normalizer_affine_rows,
):
    row_count = acoustic_features.shape[0]
    positions = lax.broadcasted_iota(jnp.int32, (row_count, 1), 0)
    slot_ends = jnp.cumsum(utterance_durations[0])
    segment = jnp.sum((positions >= slot_ends[None, :]).astype(jnp.int32), axis=1)
    valid = (positions < slot_ends[-1]).astype(jnp.float32)
    inputs = acoustic_features.astype(jnp.float32)
    taps = channelwise_kernel_weights.shape[0]
    gain_rows = normalizer_gains.shape[0]
    small = jnp.concatenate(
        [normalizer_gains, channelwise_kernel_weights, normalizer_affine_rows], axis=0
    )
    small_rows = small.shape[0]
    padding = -small_rows % 16
    small = jnp.pad(small, ((0, padding), (0, 0)))
    parts = lax.axis_size("narrow")
    order = (
        heads_merging_projector,
        gated_channel_projector,
        query_key_value_projector,
        early_expanding_projector,
        early_contracting_projector,
        later_expanding_projector,
        later_contracting_projector,
        closing_channel_projector,
        vocabulary_affinity_projector,
        vocabulary_vectors,
        small,
    )
    (
        attention_out,
        pointwise_in,
        attention_in,
        first_up,
        first_down,
        second_up,
        second_down,
        pointwise_out,
        quantizer_in,
        codebook,
        small_blocks,
    ) = gather_all(order, chunks_of(order, (1, 2, 2, 2, 2, 2, 2, 0, 0, 0, 0)))
    small_whole = (
        jnp.transpose(small_blocks.reshape(parts, small_rows + padding, -1), (1, 0, 2))
        .reshape(small_rows + padding, -1)
        .astype(jnp.float32)
    )
    gains = small_whole[:gain_rows]
    conv_small = jnp.concatenate([gains[3:4], small_whole[gain_rows:small_rows]], axis=0)

    quantizer_normed, quantizer_hat, quantizer_scale = layer_norm(inputs, gains[0])
    quantizer_entry = quantizer_normed.astype(jnp.bfloat16)
    vocabulary_affinity = matmul(quantizer_entry, quantizer_in)
    code_probabilities = jax.nn.softmax(
        (vocabulary_affinity + perturbation_samples.astype(jnp.float32)) / annealing_level[0],
        axis=-1,
    )
    chances_low = code_probabilities.astype(jnp.bfloat16)
    codes = matmul(chances_low, codebook).astype(jnp.bfloat16)
    adjoint_codes = quantized_cotangent * valid.astype(jnp.bfloat16)
    adjoint_chances = against(adjoint_codes, codebook)
    adjoint_logits = (
        code_probabilities
        * (adjoint_chances - jnp.sum(code_probabilities * adjoint_chances, axis=-1, keepdims=True))
        / annealing_level[0]
    ).astype(jnp.bfloat16)
    adjoint_inputs, quantizer_gain_sum = norm_back(
        against(adjoint_logits, quantizer_in), quantizer_hat, quantizer_scale, gains[0]
    )

    after_first, first_kept = feed_forward(inputs, first_up, first_down, gains[1])
    after_attention, attend_kept = attention_forward(
        after_first, attention_in, attention_out, gains[2], segment, HEADS
    )
    after_conv, conv_kept = convolution_forward(
        after_attention, pointwise_in, pointwise_out, conv_small, segment, valid
    )
    after_second, second_kept = feed_forward(after_conv, second_up, second_down, gains[4])
    final_out, final_hat, final_scale = layer_norm(after_second, gains[5])
    output = final_out.astype(jnp.bfloat16)

    adjoint_output = result_cotangent.astype(jnp.float32) * valid
    adjoint, final_gain_sum = norm_back(adjoint_output, final_hat, final_scale, gains[5])
    adjoint, second_up_pair, second_down_pair, second_gain_sum = feed_back(
        adjoint, second_kept, second_up, second_down, gains[4]
    )
    adjoint, pointwise_in_pair, pointwise_out_pair, conv_small_sum = convolution_back(
        adjoint, conv_kept, pointwise_in, pointwise_out, conv_small, segment, valid
    )
    adjoint, attention_in_pair, attention_out_pair, attend_gain_sum = attention_back(
        adjoint, attend_kept, attention_in, attention_out, gains[2], segment, HEADS
    )
    adjoint, first_up_pair, first_down_pair, first_gain_sum = feed_back(
        adjoint, first_kept, first_up, first_down, gains[1]
    )
    frames_gradient = (adjoint + adjoint_inputs).astype(jnp.bfloat16)
    small_sums = jnp.concatenate(
        [
            quantizer_gain_sum[None],
            first_gain_sum[None],
            attend_gain_sum[None],
            conv_small_sum[:1],
            second_gain_sum[None],
            final_gain_sum[None],
            conv_small_sum[1:],
        ],
        axis=0,
    )
    (
        first_up_gradient,
        first_down_gradient,
        attention_in_gradient,
        attention_out_gradient,
        pointwise_in_gradient,
        pointwise_out_gradient,
        second_up_gradient,
        second_down_gradient,
        quantizer_in_gradient,
        codebook_gradient,
        small_gradients,
    ) = gradients(
        (
            first_up_pair,
            first_down_pair,
            attention_in_pair,
            attention_out_pair,
            pointwise_in_pair,
            pointwise_out_pair,
            second_up_pair,
            second_down_pair,
            (quantizer_entry, adjoint_logits),
            (chances_low, adjoint_codes),
        ),
        jnp.pad(small_sums, ((0, padding), (0, 0))),
    )
    small_gradient = jnp.sum(small_gradients, axis=0) / float(lax.axis_size("wide"))
    norm_gains_gradient = small_gradient[:gain_rows]
    depthwise_kernel_gradient = small_gradient[gain_rows : gain_rows + taps]
    batch_affine_gradient = small_gradient[gain_rows + taps : small_rows]
    return (
        output,
        codes,
        frames_gradient,
        first_up_gradient,
        first_down_gradient,
        attention_in_gradient,
        attention_out_gradient,
        pointwise_in_gradient,
        pointwise_out_gradient,
        second_up_gradient,
        second_down_gradient,
        quantizer_in_gradient,
        codebook_gradient,
        norm_gains_gradient,
        depthwise_kernel_gradient,
        batch_affine_gradient,
    )


def solution(mesh):
    in_specs = (
        P(("wide", "narrow"), None),
        P(("wide", "narrow"), None),
        P(("wide", "narrow"), None),
        P(),
        P(("wide", "narrow"), None),
        P(("wide", "narrow"), None),
        P("narrow", None),
        P("narrow", None),
        P("narrow", None),
        P("narrow", None),
        P("narrow", None),
        P("narrow", None),
        P("narrow", None),
        P("narrow", None),
        P("narrow", None),
        P("narrow", None),
        P(None, "narrow"),
        P(None, "narrow"),
        P(None, "narrow"),
    )
    out_specs = (
        P(("wide", "narrow"), None),
        P(("wide", "narrow"), None),
        P(("wide", "narrow"), None),
        P("narrow", None),
        P("narrow", None),
        P("narrow", None),
        P("narrow", None),
        P("narrow", None),
        P("narrow", None),
        P("narrow", None),
        P("narrow", None),
        P("narrow", None),
        P("narrow", None),
        P(None, "narrow"),
        P(None, "narrow"),
        P(None, "narrow"),
    )
    return jax.shard_map(
        per_device, mesh=mesh, in_specs=in_specs, out_specs=out_specs, check_vma=False
    )
```

```python
import functools

import jax
import jax.numpy as jnp
from jax import lax
from jax.experimental import pallas as pl
from jax.experimental.pallas import tpu as pltpu
from jax.sharding import PartitionSpec as P

HEADS = 8
MESH = pl.DeviceIdType.MESH

EPSILON = 1e-05
NEGATIVE = -1e30


def flipped(index, bit):
    step = 1 << bit
    return index + step * (1 - 2 * ((index // step) % 2))


def bit_of(index, bit):
    return (index // (1 << bit)) % 2


def bits_of(size):
    return size.bit_length() - 1


LAG = 2


def gather_kernel(plan, *refs):
    count = (len(refs) - 4) // 3
    shards, wholes = refs[:count], refs[count : 2 * count]
    send, recv, own_in, own_out = refs[2 * count : 2 * count + 4]
    held = refs[2 * count + 4 :]
    me, wide = lax.axis_index("narrow"), lax.axis_index("wide")
    near, far = {"narrow": flipped(me, 0)}, {"narrow": flipped(me, 1)}
    across = flipped(me, 1)
    sides = ({"wide": flipped(wide, 0)}, {"wide": flipped(wide, 1)})
    side_bits = (bit_of(wide, 0), bit_of(wide, 1))
    barrier = pltpu.get_barrier_semaphore()
    for peer in (near, far) + sides:
        pl.semaphore_signal(barrier, inc=1, device_id=peer, device_id_type=MESH)
    pl.semaphore_wait(barrier, 4)
    started = []

    def start(chunk, slot, src, dst, peer):
        copy = pltpu.make_async_remote_copy(
            src_ref=src,
            dst_ref=dst,
            send_sem=send.at[chunk, slot],
            recv_sem=recv.at[chunk, slot],
            device_id=peer,
            device_id_type=MESH,
        )
        copy.start()
        started.append(copy)
        return copy

    def rows(k, block, first, size):
        begin = pl.multiple_of(block * shards[k].shape[0] + first, 16)
        return wholes[k].at[pl.ds(begin, size)]

    crossing, routes = [], []
    turn = 0
    for chunk, (k, begin, size, direct) in enumerate(plan):
        if direct:
            routes.append(None)
            piece = shards[k].at[pl.ds(begin, size)]
            crossing.append(start(chunk, 0, piece, rows(k, me, begin, size), far))
        else:
            a, b = turn, 1 - turn
            turn = b
            quarter = size // 4
            first = begin + (side_bits[b] * 2 + side_bits[a]) * quarter
            routes.append((a, b, quarter, first))
            piece = shards[k].at[pl.ds(pl.multiple_of(first, 16), quarter)]
            crossing.append(start(chunk, 0, piece, rows(k, me, first, quarter), far))
    taken = [pltpu.make_async_copy(shards[k], held[k], own_in.at[k]) for k in range(count)]
    for copy in taken:
        copy.start()
    own = [
        start(len(plan) + k, 0, shards[k], rows(k, me, 0, shards[k].shape[0]), near)
        for k in range(count)
    ]
    placed, second, third, last = [], {}, {}, []
    for step in range(len(plan) + 2 * LAG):
        if step < count:
            taken[step].wait()
            depth = shards[step].shape[0]
            placed.append(
                pltpu.make_async_copy(held[step], rows(step, me, 0, depth), own_out.at[step])
            )
            placed[-1].start()
        chunk = step - 2 * LAG
        if chunk in third:
            third[chunk].wait_recv()
            k, begin, size, _ = plan[chunk]
            a, b, quarter, first = routes[chunk]
            block = rows(k, across, begin + (1 - side_bits[b]) * 2 * quarter, 2 * quarter)
            last.append(start(chunk, 5, block, block, near))
        chunk = step - LAG
        if chunk in second:
            second[chunk].wait_recv()
            k, begin, size, _ = plan[chunk]
            a, b, quarter, first = routes[chunk]
            block = rows(k, across, begin + side_bits[b] * 2 * quarter, 2 * quarter)
            third[chunk] = start(chunk, 3, block, block, sides[b])
            last.append(start(chunk, 4, block, block, near))
        chunk = step
        if chunk < len(plan):
            crossing[chunk].wait_recv()
            k, begin, size, direct = plan[chunk]
            if direct:
                block = rows(k, across, begin, size)
                last.append(start(chunk, 2, block, block, near))
            else:
                a, b, quarter, first = routes[chunk]
                block = rows(k, across, first, quarter)
                second[chunk] = start(chunk, 2, block, block, sides[a])
    for copy in own + last:
        copy.wait_recv()
    for copy in started:
        copy.wait_send()
    for copy in placed:
        copy.wait()


def chunks_of(shards, pieces):
    plan = []
    for k, (shard, cuts) in enumerate(zip(shards, pieces)):
        size = shard.shape[0] // max(cuts, 1)
        plan += [(k, i * size, size, cuts == 0) for i in range(max(cuts, 1))]
    return tuple(plan)


def gather_all(shards, plan):
    count = len(shards)
    parts = lax.axis_size("narrow")
    return pl.pallas_call(
        functools.partial(gather_kernel, plan),
        out_shape=[
            jax.ShapeDtypeStruct((shard.shape[0] * parts, shard.shape[1]), shard.dtype)
            for shard in shards
        ],
        in_specs=[pl.BlockSpec(memory_space=pl.ANY)] * count,
        out_specs=[pl.BlockSpec(memory_space=pl.ANY)] * count,
        scratch_shapes=[
            pltpu.SemaphoreType.DMA((len(plan) + count, 6)),
            pltpu.SemaphoreType.DMA((len(plan) + count, 6)),
            pltpu.SemaphoreType.DMA((count,)),
            pltpu.SemaphoreType.DMA((count,)),
        ]
        + [pltpu.VMEM(shard.shape, shard.dtype) for shard in shards],
        compiler_params=pltpu.CompilerParams(collective_id=0, has_side_effects=True),
    )(*shards)


def exchange_all(across, within, mine_ref, all_ref, send, recv):
    total = across * within
    me = lax.axis_index("wide") * within + lax.axis_index("narrow")

    def peer_of(step):
        peer = lax.rem(me + step, total)
        return (peer // within, lax.rem(peer, within))

    barrier = pltpu.get_barrier_semaphore()

    def greet(step, carry):
        pl.semaphore_signal(barrier, inc=1, device_id=peer_of(step), device_id_type=MESH)
        return carry

    lax.fori_loop(1, total, greet, 0)

    def copy_of(step):
        return pltpu.make_async_remote_copy(
            src_ref=mine_ref,
            dst_ref=all_ref.at[me],
            send_sem=send.at[step],
            recv_sem=recv.at[step],
            device_id=peer_of(step),
            device_id_type=MESH,
        )

    def begin(step, carry):
        copy_of(step).start()
        return carry

    def finish(step, carry):
        copy_of(step).wait()
        return carry

    def run():
        pl.semaphore_wait(barrier, total - 1)
        lax.fori_loop(1, total, begin, 0)
        all_ref[me] = mine_ref[...]
        lax.fori_loop(1, total, finish, 0)

    return run


LANES = 128


def row_masks(segments, taps, masks):
    rows = segments.shape[0]
    segment = jnp.broadcast_to(segments[...], (rows, LANES))
    position = lax.broadcasted_iota(jnp.int32, (rows, LANES), 0)
    for tap in range(taps):
        offset = tap - taps // 2
        there = pltpu.roll(segment, -offset % rows, 0) if offset else segment
        inside = (position + offset >= 0) & (position + offset < rows)
        masks[tap] = jnp.where(inside & (there == segment), 1.0, 0.0)


def moved(value, offset):
    return pltpu.roll(value, -offset % value.shape[0], 0) if offset else value


def convolve_kernel(
    across, within, taps, gates, segments, valids, small, active, hats, stats,
    mine, everyone, convolved, masks, send, recv,
):
    share = exchange_all(across, within, mine, everyone, send, recv)
    rows, width = hats.shape
    chunks = width // LANES
    row_masks(segments, taps, masks)
    valid = jnp.broadcast_to(valids[...], (rows, LANES))
    here = jnp.sum(valid, axis=0, keepdims=True)
    mine[2 * chunks : 2 * chunks + 1, :] = here
    for chunk in range(chunks):
        at = pl.ds(chunk * LANES, LANES)
        gated = gates[:, at] * jax.nn.sigmoid(gates[:, pl.ds(width + chunk * LANES, LANES)])
        total = jnp.zeros_like(gated)
        for tap in range(taps):
            total += small[1 + tap : 2 + tap, at] * moved(gated, tap - taps // 2) * masks[tap]
        convolved[:, at] = total
        summed = jnp.sum(total * valid, axis=0, keepdims=True)
        off = (total - summed / jnp.maximum(here, 1.0)) * valid
        mine[chunk : chunk + 1, :] = summed
        mine[chunks + chunk : chunks + chunk + 1, :] = jnp.sum(off * off, axis=0, keepdims=True)
    share()
    counts = everyone[:, 2 * chunks, :]
    count = jnp.sum(counts, axis=0, keepdims=True)
    for chunk in range(chunks):
        at = pl.ds(chunk * LANES, LANES)
        totals = everyone[:, chunk, :]
        mean = jnp.sum(totals, axis=0, keepdims=True) / count
        apart = totals / jnp.maximum(counts, 1.0) - mean
        squares = everyone[:, chunks + chunk, :] + counts * apart * apart
        inverse = lax.rsqrt(jnp.sum(squares, axis=0, keepdims=True) / count + EPSILON)
        stats[0:1, at] = inverse
        stats[1:2, at] = count
        hat = (convolved[:, at] - mean) * inverse
        hats[:, at] = hat
        out = hat * small[1 + taps : 2 + taps, at] + small[2 + taps : 3 + taps, at]
        active[:, at] = (out * jax.nn.sigmoid(out)).astype(jnp.bfloat16)


def convolve_back_kernel(
    across, within, taps, adjoint, gates, hats, stats, segments, valids, small, adjoint_gates, sums,
    mine, everyone, adjoint_hats, masks, send, recv,
):
    share = exchange_all(across, within, mine, everyone, send, recv)
    rows, width = hats.shape
    chunks = width // LANES
    row_masks(segments, taps, masks)
    valid = jnp.broadcast_to(valids[...], (rows, LANES))
    for chunk in range(chunks):
        at = pl.ds(chunk * LANES, LANES)
        hat, gain = hats[:, at], small[1 + taps : 2 + taps, at]
        adjoint_batch = adjoint[:, at] * swish_slope(hat * gain + small[2 + taps : 3 + taps, at])
        sums[taps : taps + 1, at] = jnp.sum(adjoint_batch * hat, axis=0, keepdims=True)
        sums[taps + 1 : taps + 2, at] = jnp.sum(adjoint_batch, axis=0, keepdims=True)
        adjoint_hat = adjoint_batch * gain
        adjoint_hats[:, at] = adjoint_hat
        counted = adjoint_hat * valid
        mine[chunk : chunk + 1, :] = jnp.sum(counted, axis=0, keepdims=True)
        mine[chunks + chunk : chunks + chunk + 1, :] = jnp.sum(counted * hat, axis=0, keepdims=True)
    share()
    for chunk in range(chunks):
        at = pl.ds(chunk * LANES, LANES)
        right_at = pl.ds(width + chunk * LANES, LANES)
        first = jnp.sum(everyone[:, chunk, :], axis=0, keepdims=True)
        second = jnp.sum(everyone[:, chunks + chunk, :], axis=0, keepdims=True)
        adjoint_conv = stats[0:1, at] * (
            adjoint_hats[:, at] - valid * (first + hats[:, at] * second) / stats[1:2, at]
        )
        sigmoid, left = jax.nn.sigmoid(gates[:, right_at]), gates[:, at]
        gated = left * sigmoid
        adjoint_gated = jnp.zeros_like(gated)
        for tap in range(taps):
            offset = tap - taps // 2
            masked = adjoint_conv * masks[tap]
            sums[tap : tap + 1, at] = jnp.sum(masked * moved(gated, offset), axis=0, keepdims=True)
            adjoint_gated += moved(masked * small[1 + tap : 2 + tap, at], -offset)
        adjoint_gates[:, at] = (adjoint_gated * sigmoid).astype(jnp.bfloat16)
        adjoint_gates[:, right_at] = (adjoint_gated * gated * (1.0 - sigmoid)).astype(jnp.bfloat16)


def convolution_call(kernel, identity, inputs, out_shape, shared_rows, taps):
    across, within = lax.axis_size("wide"), lax.axis_size("narrow")
    rows, width = inputs[0].shape[0], out_shape[1].shape[1]
    here = pl.BlockSpec(memory_space=pltpu.VMEM)
    high = jnp.float32
    return pl.pallas_call(
        functools.partial(kernel, across, within, taps),
        out_shape=out_shape,
        in_specs=[here] * len(inputs),
        out_specs=[here] * len(out_shape),
        scratch_shapes=[
            pltpu.VMEM((shared_rows, LANES), high),
            pltpu.VMEM((across * within, shared_rows, LANES), high),
            pltpu.VMEM((rows, width), high),
            pltpu.VMEM((taps, rows, LANES), high),
            pltpu.SemaphoreType.DMA((across * within,)),
            pltpu.SemaphoreType.DMA((across * within,)),
        ],
        compiler_params=pltpu.CompilerParams(collective_id=identity, has_side_effects=True),
    )(*inputs)


def columns_split(small, pieces):
    rows, width = small.shape
    split = jnp.transpose(small.reshape(rows, pieces, width // pieces), (1, 0, 2))
    return split.reshape(pieces, rows * width // pieces // 128, 128)


COLS = 256
ROWS = 256
LAGS = 16


def gradient_kernel(plan, extra, across, within, *refs):
    count = len(plan)
    lefts, rights = refs[:count], refs[count : 2 * count]
    small, outs, smalls = refs[2 * count], refs[2 * count + 1 : 3 * count + 1], refs[3 * count + 1]
    (
        left_buf,
        right_buf,
        near_send,
        near_recv,
        held,
        far_send,
        far_recv,
        kept,
        half_send,
        half_recv,
        half_kept,
        quarter_send,
        quarter_recv,
        quarter_kept,
        eighth_send,
        eighth_recv,
        eighth_kept,
        whole_send,
        whole_recv,
        back_eighth,
        back_eighth_recv,
        back_quarter,
        back_quarter_recv,
        back_half,
        back_half_recv,
        out_buf,
        fetch_sem,
        out_sem,
        sends,
        recvs,
        small_send,
        small_recv,
    ) = refs[3 * count + 2 :]
    total = sum(units for _, units, _, _ in plan)
    me, wide = lax.axis_index("narrow"), lax.axis_index("wide")
    core, side = bit_of(me, 0), bit_of(me, 1)
    near, far = {"narrow": flipped(me, 0)}, {"narrow": flipped(me, 1)}
    bits = [bit_of(wide, i) for i in range(3)]
    devices = across * within
    place = wide * within + me

    def peer_of(step):
        peer = lax.rem(place + step, devices)
        return (peer // within, lax.rem(peer, within))

    barrier = pltpu.get_barrier_semaphore()

    def greet(step, carry):
        pl.semaphore_signal(barrier, inc=1, device_id=peer_of(step), device_id_type=MESH)
        return carry

    lax.fori_loop(1, devices, greet, 0)
    pl.semaphore_wait(barrier, devices - 1)

    def small_copy(step):
        return pltpu.make_async_remote_copy(
            src_ref=small.at[lax.rem(place + step, within)],
            dst_ref=smalls.at[place],
            send_sem=small_send.at[step],
            recv_sem=small_recv.at[step],
            device_id=peer_of(step),
            device_id_type=MESH,
        )

    def begin(step, carry):
        small_copy(step).start()
        return carry

    def end(step, carry):
        small_copy(step).wait()
        return carry

    def order_of(unit):
        turn = lax.rem(unit, 2)
        first = bits[0] * (1 - turn) + bits[1] * turn
        second = bits[1] * (1 - turn) + bits[0] * turn
        near_step, far_step = 1 - 2 * bits[0], 2 * (1 - 2 * bits[1])
        first_peer = {"wide": wide + near_step * (1 - turn) + far_step * turn}
        second_peer = {"wide": wide + far_step * (1 - turn) + near_step * turn}
        return first, second, bits[2], first_peer, second_peer, {"wide": flipped(wide, 2)}

    def exchange(stage, unit, slots, source, target, peer):
        slot = lax.rem(unit, slots)
        return pltpu.make_async_remote_copy(
            src_ref=source.at[slot],
            dst_ref=target.at[slot],
            send_sem=sends.at[stage, slot],
            recv_sem=recvs.at[stage, slot],
            device_id=peer,
            device_id_type=MESH,
        )

    def fetches(i, unit, slot):
        first, _, width, per_row = plan[i]
        place = unit - first
        deep, col = place // per_row, lax.rem(place, per_row)
        copies = []
        for n in range(4):
            begin = pl.multiple_of(n * (width // 4) + deep * ROWS, ROWS)
            copies.append(
                pltpu.make_async_copy(
                    lefts[i].at[:, pl.ds(begin, ROWS)],
                    left_buf.at[slot, n],
                    fetch_sem.at[slot, n],
                )
            )
        begin = pl.multiple_of(col * COLS, COLS)
        copies.append(
            pltpu.make_async_copy(
                rights[i].at[:, pl.ds(begin, COLS)], right_buf.at[slot], fetch_sem.at[slot, 4]
            )
        )
        return copies

    def fetch(unit):
        for i, (first, units, _, _) in enumerate(plan):

            @pl.when((unit >= first) & (unit < first + units))
            def _(i=i):
                for copy in fetches(i, unit, lax.rem(unit, 2)):
                    copy.start()

    def placing(i, unit, slot):
        first, _, _, per_row = plan[i]
        place = unit - first
        deep, col = place // per_row, lax.rem(place, per_row)
        block = outs[i].at[
            pl.ds(pl.multiple_of(deep * ROWS, ROWS), ROWS),
            pl.ds(pl.multiple_of(col * COLS, COLS), COLS),
        ]
        return pltpu.make_async_copy(out_buf.at[slot], block, out_sem.at[slot])

    def by_rows(rows, body):
        def step(r, carry):
            body(pl.multiple_of(r * 32, 32))
            return carry

        if rows == 32:
            body(0)
        else:
            lax.fori_loop(0, rows // 32, step, 0)

    def added(first, first_slot, first_row, second, second_slot, second_row):
        return first[first_slot, pl.ds(first_row, 32), :].astype(jnp.float32) + second[
            second_slot, pl.ds(second_row, 32), :
        ].astype(jnp.float32)

    def stage_of(lag, tick, body):
        unit = tick - lag

        @pl.when((unit >= 0) & (unit < total))
        def _():
            body(unit)

    def split(unit, rows, bit, kept_in, arrived, slot, send_to, keep_in):
        half = rows // 2

        def body(r):
            theirs, mine = (1 - bit) * half + r, bit * half + r
            send_to[slot, pl.ds(r, 32), :] = added(
                kept_in, slot, theirs, arrived, slot, theirs
            ).astype(jnp.bfloat16)
            keep_in[slot, pl.ds(r, 32), :] = added(kept_in, slot, mine, arrived, slot, mine)

        by_rows(half, body)

    def joined(rows, bit, mine, arrived, slot, target):
        half = rows // 2

        def body(r):
            target[slot, pl.ds(bit * half + r, 32), :] = mine[slot, pl.ds(r, 32), :]
            target[slot, pl.ds((1 - bit) * half + r, 32), :] = arrived[slot, pl.ds(r, 32), :]

        by_rows(half, body)

    def finish(unit):
        first, _, _, first_peer, _, _ = order_of(unit)
        exchange(7, unit, 4, back_half, back_half_recv, first_peer).wait()
        slot = lax.rem(unit, 4)

        @pl.when(unit >= 4)
        def _():
            placing(0, unit * 0, slot).wait()

        joined(
            ROWS, first, back_half, back_half_recv, slot, out_buf,
        )
        for i, (start, units, _, _) in enumerate(plan):

            @pl.when((unit >= start) & (unit < start + units))
            def _(i=i):
                placing(i, unit, slot).start()

    def double_last(unit):
        _, second, _, first_peer, second_peer, _ = order_of(unit)
        exchange(6, unit, 4, back_quarter, back_quarter_recv, second_peer).wait()
        joined(
            ROWS // 2, second, back_quarter, back_quarter_recv, lax.rem(unit, 4), back_half,
        )
        exchange(7, unit, 4, back_half, back_half_recv, first_peer).start()

    def double_first(unit):
        _, _, third, _, second_peer, third_peer = order_of(unit)
        exchange(5, unit, 4, back_eighth, back_eighth_recv, third_peer).wait()
        joined(
            ROWS // 4, third, back_eighth, back_eighth_recv, lax.rem(unit, 4), back_quarter,
        )
        exchange(6, unit, 4, back_quarter, back_quarter_recv, second_peer).start()

    def turn_back(unit):
        _, _, _, _, _, third_peer = order_of(unit)
        slot = lax.rem(unit, 4)
        exchange(4, unit, 4, eighth_send, eighth_recv, third_peer).wait()
        value = added(eighth_kept, slot, 0, eighth_recv, slot, 0)
        for bit in range(3, 3 + extra):
            whole_send[slot] = value.astype(jnp.bfloat16)
            copy = exchange(5 + bit, unit, 4, whole_send, whole_recv.at[bit - 3], {"wide": flipped(wide, bit)})
            copy.start()
            copy.wait()
            value = value + whole_recv[bit - 3, slot].astype(jnp.float32)
        back_eighth[slot] = value.astype(jnp.bfloat16)
        exchange(5, unit, 4, back_eighth, back_eighth_recv, third_peer).start()

    def halve_third(unit):
        _, _, third, _, second_peer, third_peer = order_of(unit)
        slot = lax.rem(unit, 4)
        exchange(3, unit, 4, quarter_send, quarter_recv, second_peer).wait()
        split(unit, ROWS // 4, third, quarter_kept, quarter_recv, slot, eighth_send, eighth_kept)
        exchange(4, unit, 4, eighth_send, eighth_recv, third_peer).start()

    def halve_second(unit):
        _, second, _, first_peer, second_peer, _ = order_of(unit)
        slot = lax.rem(unit, 4)
        exchange(2, unit, 4, half_send, half_recv, first_peer).wait()
        split(unit, ROWS // 2, second, half_kept, half_recv, slot, quarter_send, quarter_kept)
        exchange(3, unit, 4, quarter_send, quarter_recv, second_peer).start()

    def halve_first(unit):
        first, _, _, first_peer, _, _ = order_of(unit)
        slot = lax.rem(unit, 4)
        exchange(1, unit, 4, far_send, far_recv, far).wait()
        split(unit, ROWS, first, kept, far_recv, slot, half_send, half_kept)
        exchange(2, unit, 4, half_send, half_recv, first_peer).start()

    def cross(unit):
        slot, near_slot = lax.rem(unit, 4), lax.rem(unit, 2)
        exchange(0, unit, 2, near_send, near_recv, near).wait()

        def body(r):
            far_send[slot, pl.ds(r, 32), :] = (
                held[near_slot, 0, pl.ds(r, 32), :]
                + near_recv[near_slot, 0, pl.ds(r, 32), :].astype(jnp.float32)
            ).astype(jnp.bfloat16)
            kept[slot, pl.ds(r, 32), :] = held[near_slot, 1, pl.ds(r, 32), :] + near_recv[
                near_slot, 1, pl.ds(r, 32), :
            ].astype(jnp.float32)

        by_rows(ROWS, body)
        exchange(1, unit, 4, far_send, far_recv, far).start()

    def multiply(unit):
        slot = lax.rem(unit, 2)
        for copy in fetches(0, unit * 0, slot):
            copy.wait()

        @pl.when(unit + 1 < total)
        def _():
            fetch(unit + 1)

        def product(block, first):
            return lax.dot_general(
                left_buf[slot, block],
                right_buf[slot, :, pl.ds(first, 256)],
                (((0,), (0,)), ((), ())),
                preferred_element_type=jnp.float32,
            )

        for which in range(2):
            block = 2 * (side * which + (1 - side) * (1 - which)) + 1 - core
            for first in range(0, COLS, 256):
                near_send[slot, which, :, pl.ds(first, 256)] = product(block, first).astype(
                    jnp.bfloat16
                )
        exchange(0, unit, 2, near_send, near_recv, near).start()
        for which in range(2):
            block = 2 * (side * which + (1 - side) * (1 - which)) + core
            for first in range(0, COLS, 256):
                held[slot, which, :, pl.ds(first, 256)] = product(block, first)

    fetch(me * 0)
    lax.fori_loop(1, devices, begin, 0)
    smalls[place] = small[me]

    def tick(step, carry):
        stage_of(15, step, finish)
        stage_of(13, step, double_last)
        stage_of(11, step, double_first)
        stage_of(9, step, turn_back)
        stage_of(7, step, halve_third)
        stage_of(5, step, halve_second)
        stage_of(3, step, halve_first)
        stage_of(1, step, cross)
        stage_of(0, step, multiply)
        return carry

    lax.fori_loop(0, total + LAGS - 1, tick, 0)
    for slot in range(4):
        placing(0, me * 0, slot).wait()
    lax.fori_loop(1, devices, end, 0)


def gradients(pairs, small):
    parts, copies = lax.axis_size("narrow"), lax.axis_size("wide")
    extra = bits_of(copies) - 3
    plan, begun = [], 0
    for left, right in pairs:
        per_row = right.shape[1] // COLS
        units = per_row * (left.shape[1] // (parts * ROWS))
        plan.append((begun, units, left.shape[1], per_row))
        begun += units
    rows = pairs[0][0].shape[0]
    low, high = jnp.bfloat16, jnp.float32

    def pair_of(size, slots=4):
        return [pltpu.VMEM((slots, size, COLS), low)] * 2

    def trio_of(size):
        return pair_of(size) + [pltpu.VMEM((4, size, COLS), high)]

    scratch = (
        [
            pltpu.VMEM((2, 4, rows, ROWS), low),
            pltpu.VMEM((2, rows, COLS), low),
            pltpu.VMEM((2, 2, ROWS, COLS), low),
            pltpu.VMEM((2, 2, ROWS, COLS), low),
            pltpu.VMEM((2, 2, ROWS, COLS), high),
        ]
        + trio_of(ROWS)
        + trio_of(ROWS // 2)
        + trio_of(ROWS // 4)
        + trio_of(ROWS // 8)
        + [
            pltpu.VMEM((4, ROWS // 8, COLS), low),
            pltpu.VMEM((max(extra, 1), 4, ROWS // 8, COLS), low),
        ]
        + pair_of(ROWS // 8)
        + pair_of(ROWS // 4)
        + pair_of(ROWS // 2)
        + [
            pltpu.VMEM((4, ROWS, COLS), low),
            pltpu.SemaphoreType.DMA((2, 5)),
            pltpu.SemaphoreType.DMA((4,)),
            pltpu.SemaphoreType.DMA((8 + extra, 4)),
            pltpu.SemaphoreType.DMA((8 + extra, 4)),
            pltpu.SemaphoreType.DMA((copies * parts,)),
            pltpu.SemaphoreType.DMA((copies * parts,)),
        ]
    )
    count = len(pairs)
    split = columns_split(small, parts)
    results = pl.pallas_call(
        functools.partial(gradient_kernel, tuple(plan), extra, copies, parts),
        out_shape=[
            jax.ShapeDtypeStruct((left.shape[1] // parts, right.shape[1]), low)
            for left, right in pairs
        ]
        + [jax.ShapeDtypeStruct((copies * parts,) + split.shape[1:], high)],
        in_specs=[pl.BlockSpec(memory_space=pl.ANY)] * (2 * count)
        + [pl.BlockSpec(memory_space=pltpu.VMEM)],
        out_specs=[pl.BlockSpec(memory_space=pl.ANY)] * count
        + [pl.BlockSpec(memory_space=pltpu.VMEM)],
        scratch_shapes=scratch,
        compiler_params=pltpu.CompilerParams(collective_id=4, has_side_effects=True),
    )(*[left for left, _ in pairs], *[right for _, right in pairs], split)
    everyone = results[-1].reshape(copies * parts, small.shape[0], -1)
    return tuple(whole.astype(high) / float(copies) for whole in results[:-1]) + (everyone,)


def matmul(left, right):
    return jnp.dot(left, right, preferred_element_type=jnp.float32)


def across_rows(left, right):
    return lax.dot_general(
        left, right, (((0,), (0,)), ((), ())), preferred_element_type=jnp.float32
    )


def against(left, right):
    return lax.dot_general(
        left, right, (((1,), (1,)), ((), ())), preferred_element_type=jnp.float32
    )


def swish_slope(values):
    sigmoid = jax.nn.sigmoid(values)
    return sigmoid * (1.0 + values * (1.0 - sigmoid))


def layer_norm(values, gain):
    centred = values - jnp.mean(values, axis=-1, keepdims=True)
    scale = lax.rsqrt(jnp.mean(centred * centred, axis=-1, keepdims=True) + EPSILON)
    normed = centred * scale
    return (normed * gain, normed, scale)


def norm_back(adjoint_out, normed, scale, gain):
    adjoint_normed = adjoint_out * gain
    gain_sum = jnp.sum(adjoint_out * normed, axis=0)
    adjoint_in = scale * (
        adjoint_normed
        - jnp.mean(adjoint_normed, axis=-1, keepdims=True)
        - normed * jnp.mean(adjoint_normed * normed, axis=-1, keepdims=True)
    )
    return (adjoint_in, gain_sum)


def feed_forward(values, weight_in, weight_out, gain):
    normed, normal_hat, scale = layer_norm(values, gain)
    entry = normed.astype(jnp.bfloat16)
    before = matmul(entry, weight_in)
    active = (before * jax.nn.sigmoid(before)).astype(jnp.bfloat16)
    branch = matmul(active, weight_out)
    return (values + 0.5 * branch, (entry, normal_hat, scale, before, active))


def feed_back(adjoint, kept, weight_in, weight_out, gain):
    entry, normal_hat, scale, before, active = kept
    adjoint_branch = (0.5 * adjoint).astype(jnp.bfloat16)
    adjoint_before = (against(adjoint_branch, weight_out) * swish_slope(before)).astype(
        jnp.bfloat16
    )
    adjoint_values, gain_sum = norm_back(
        against(adjoint_before, weight_in), normal_hat, scale, gain
    )
    return (
        adjoint + adjoint_values,
        (entry, adjoint_before),
        (active, adjoint_branch),
        gain_sum,
    )


def head_weights(query, key, rows, columns, factor):
    scores = against(query, key) * factor
    scores = jnp.where(rows == columns, scores, NEGATIVE)
    exponent = jnp.exp(scores - jnp.max(scores, axis=-1, keepdims=True))
    return exponent / jnp.sum(exponent, axis=-1, keepdims=True)


def attend_kernel(factor, query, key, value, rows, columns, result):
    weights = head_weights(query[...], key[...], rows[...], columns[...], factor)
    result[...] = matmul(weights.astype(jnp.bfloat16), value[...]).astype(jnp.bfloat16)


def attend_back_kernel(factor, heads, query, key, value, adjoint, rows, columns, result):
    weights = head_weights(query[...], key[...], rows[...], columns[...], factor)
    adjoint_weights = against(adjoint[...], value[...])
    inner = jnp.sum(weights * adjoint_weights, axis=-1, keepdims=True)
    adjoint_scores = (weights * (adjoint_weights - inner)).astype(jnp.bfloat16)
    head_dim = query.shape[1]
    head = pl.program_id(0)
    for place, part in enumerate(
        (
            matmul(adjoint_scores, key[...]) * factor,
            across_rows(adjoint_scores, query[...]) * factor,
            across_rows(weights.astype(jnp.bfloat16), adjoint[...]),
        )
    ):
        at = pl.multiple_of((place * heads + head) * head_dim, head_dim)
        result[:, pl.ds(at, head_dim)] = part.astype(jnp.bfloat16)


def over_heads(kernel, mixed, extra, segment, heads, out_shape, out_spec, products):
    row_count = mixed.shape[0]
    head_dim = mixed.shape[1] // 3 // heads

    def block(place):
        return pl.BlockSpec((row_count, head_dim), lambda head: (0, place * heads + head))

    return pl.pallas_call(
        kernel,
        grid=(heads,),
        out_shape=out_shape,
        in_specs=[block(0), block(1), block(2)]
        + [block(0)] * len(extra)
        + [
            pl.BlockSpec((row_count, 1), lambda head: (0, 0)),
            pl.BlockSpec((1, row_count), lambda head: (0, 0)),
        ],
        out_specs=out_spec,
        cost_estimate=pl.CostEstimate(
            flops=products * 2 * heads * row_count * row_count * head_dim,
            bytes_accessed=16 * row_count * heads * head_dim,
            transcendentals=heads * row_count * row_count,
        ),
    )(mixed, mixed, mixed, *extra, segment[:, None], segment[None, :])


def attention_forward(values, weight_in, weight_out, gain, segment, heads):
    normed, normal_hat, scale = layer_norm(values, gain)
    entry = normed.astype(jnp.bfloat16)
    mixed = matmul(entry, weight_in).astype(jnp.bfloat16)
    row_count, width = values.shape
    head_dim = width // heads
    heads_out = over_heads(
        functools.partial(attend_kernel, head_dim ** (-0.5)),
        mixed,
        (),
        segment,
        heads,
        jax.ShapeDtypeStruct((row_count, width), jnp.bfloat16),
        pl.BlockSpec((row_count, head_dim), lambda head: (0, head)),
        2,
    )
    branch = matmul(heads_out, weight_out)
    return (values + branch, (entry, normal_hat, scale, mixed, heads_out))


def attention_back(adjoint, kept, weight_in, weight_out, gain, segment, heads):
    entry, normal_hat, scale, mixed, heads_out = kept
    head_dim = adjoint.shape[1] // heads
    adjoint_branch = adjoint.astype(jnp.bfloat16)
    adjoint_heads = against(adjoint_branch, weight_out).astype(jnp.bfloat16)
    adjoint_mixed = over_heads(
        functools.partial(attend_back_kernel, head_dim ** (-0.5), heads),
        mixed,
        (adjoint_heads,),
        segment,
        heads,
        jax.ShapeDtypeStruct(mixed.shape, jnp.bfloat16),
        pl.BlockSpec(mixed.shape, lambda head: (0, 0)),
        5,
    )
    adjoint_values, gain_sum = norm_back(against(adjoint_mixed, weight_in), normal_hat, scale, gain)
    return (
        adjoint + adjoint_values,
        (entry, adjoint_mixed),
        (heads_out, adjoint_branch),
        gain_sum,
    )


def convolution_forward(values, weight_in, weight_out, small, segment, valid):
    taps = small.shape[0] - 3
    normed, normal_hat, scale = layer_norm(values, small[0])
    entry = normed.astype(jnp.bfloat16)
    gates = matmul(entry, weight_in)
    high = jnp.float32
    columns = (segment[:, None], valid)
    active, hats, stats = convolution_call(
        convolve_kernel,
        1,
        (gates,) + columns + (small,),
        [
            jax.ShapeDtypeStruct(values.shape, jnp.bfloat16),
            jax.ShapeDtypeStruct(values.shape, high),
            jax.ShapeDtypeStruct((2, values.shape[1]), high),
        ],
        2 * values.shape[1] // LANES + 1,
        taps,
    )
    branch = matmul(active, weight_out)
    return (values + branch, (entry, normal_hat, scale, gates, hats, stats, active, columns))


def convolution_back(adjoint, kept, weight_in, weight_out, small):
    entry, normal_hat, scale, gates, hats, stats, active, columns = kept
    taps = small.shape[0] - 3
    adjoint_branch = adjoint.astype(jnp.bfloat16)
    adjoint_gates, sums = convolution_call(
        convolve_back_kernel,
        2,
        (against(adjoint_branch, weight_out), gates, hats, stats) + columns + (small,),
        [
            jax.ShapeDtypeStruct(gates.shape, jnp.bfloat16),
            jax.ShapeDtypeStruct((taps + 2, adjoint.shape[1]), jnp.float32),
        ],
        2 * adjoint.shape[1] // LANES,
        taps,
    )
    adjoint_values, gain_sum = norm_back(
        against(adjoint_gates, weight_in), normal_hat, scale, small[0]
    )
    small_sum = jnp.concatenate([gain_sum[None], sums], axis=0)
    return (adjoint + adjoint_values, (entry, adjoint_gates), (active, adjoint_branch), small_sum)


def per_device(
    acoustic_features,
    utterance_durations,
    perturbation_samples,
    annealing_level,
    result_cotangent,
    quantized_cotangent,
    early_expanding_projector,
    early_contracting_projector,
    query_key_value_projector,
    heads_merging_projector,
    gated_channel_projector,
    closing_channel_projector,
    later_expanding_projector,
    later_contracting_projector,
    vocabulary_affinity_projector,
    vocabulary_vectors,
    normalizer_gains,
    channelwise_kernel_weights,
    normalizer_affine_rows,
):
    row_count = acoustic_features.shape[0]
    positions = lax.broadcasted_iota(jnp.int32, (row_count, 1), 0)
    slot_ends = jnp.cumsum(utterance_durations[0])
    segment = jnp.sum((positions >= slot_ends[None, :]).astype(jnp.int32), axis=1)
    valid = (positions < slot_ends[-1]).astype(jnp.float32)
    inputs = acoustic_features.astype(jnp.float32)
    taps = channelwise_kernel_weights.shape[0]
    gain_rows = normalizer_gains.shape[0]
    small = jnp.concatenate(
        [normalizer_gains, channelwise_kernel_weights, normalizer_affine_rows], axis=0
    )
    small_rows = small.shape[0]
    padding = -small_rows % 16
    small = jnp.pad(small, ((0, padding), (0, 0)))
    parts = lax.axis_size("narrow")
    order = (
        heads_merging_projector,
        gated_channel_projector,
        query_key_value_projector,
        early_expanding_projector,
        early_contracting_projector,
        later_expanding_projector,
        later_contracting_projector,
        closing_channel_projector,
        vocabulary_affinity_projector,
        vocabulary_vectors,
        small,
    )
    (
        attention_out,
        pointwise_in,
        attention_in,
        first_up,
        first_down,
        second_up,
        second_down,
        pointwise_out,
        quantizer_in,
        codebook,
        small_blocks,
    ) = gather_all(order, chunks_of(order, (1, 2, 2, 2, 2, 2, 2, 0, 0, 0, 0)))
    small_whole = (
        jnp.transpose(small_blocks.reshape(parts, small_rows + padding, -1), (1, 0, 2))
        .reshape(small_rows + padding, -1)
        .astype(jnp.float32)
    )
    gains = small_whole[:gain_rows]
    conv_small = jnp.concatenate([gains[3:4], small_whole[gain_rows:small_rows]], axis=0)

    quantizer_normed, quantizer_hat, quantizer_scale = layer_norm(inputs, gains[0])
    quantizer_entry = quantizer_normed.astype(jnp.bfloat16)
    vocabulary_affinity = matmul(quantizer_entry, quantizer_in)
    code_probabilities = jax.nn.softmax(
        (vocabulary_affinity + perturbation_samples.astype(jnp.float32)) / annealing_level[0],
        axis=-1,
    )
    chances_low = code_probabilities.astype(jnp.bfloat16)
    codes = matmul(chances_low, codebook).astype(jnp.bfloat16)
    adjoint_codes = quantized_cotangent * valid.astype(jnp.bfloat16)
    adjoint_chances = against(adjoint_codes, codebook)
    adjoint_logits = (
        code_probabilities
        * (adjoint_chances - jnp.sum(code_probabilities * adjoint_chances, axis=-1, keepdims=True))
        / annealing_level[0]
    ).astype(jnp.bfloat16)
    adjoint_inputs, quantizer_gain_sum = norm_back(
        against(adjoint_logits, quantizer_in), quantizer_hat, quantizer_scale, gains[0]
    )

    after_first, first_kept = feed_forward(inputs, first_up, first_down, gains[1])
    after_attention, attend_kept = attention_forward(
        after_first, attention_in, attention_out, gains[2], segment, HEADS
    )
    after_conv, conv_kept = convolution_forward(
        after_attention, pointwise_in, pointwise_out, conv_small, segment, valid
    )
    after_second, second_kept = feed_forward(after_conv, second_up, second_down, gains[4])
    final_out, final_hat, final_scale = layer_norm(after_second, gains[5])
    output = final_out.astype(jnp.bfloat16)

    adjoint_output = result_cotangent.astype(jnp.float32) * valid
    adjoint, final_gain_sum = norm_back(adjoint_output, final_hat, final_scale, gains[5])
    adjoint, second_up_pair, second_down_pair, second_gain_sum = feed_back(
        adjoint, second_kept, second_up, second_down, gains[4]
    )
    adjoint, pointwise_in_pair, pointwise_out_pair, conv_small_sum = convolution_back(
        adjoint, conv_kept, pointwise_in, pointwise_out, conv_small
    )
    adjoint, attention_in_pair, attention_out_pair, attend_gain_sum = attention_back(
        adjoint, attend_kept, attention_in, attention_out, gains[2], segment, HEADS
    )
    adjoint, first_up_pair, first_down_pair, first_gain_sum = feed_back(
        adjoint, first_kept, first_up, first_down, gains[1]
    )
    frames_gradient = (adjoint + adjoint_inputs).astype(jnp.bfloat16)
    small_sums = jnp.concatenate(
        [
            quantizer_gain_sum[None],
            first_gain_sum[None],
            attend_gain_sum[None],
            conv_small_sum[:1],
            second_gain_sum[None],
            final_gain_sum[None],
            conv_small_sum[1:],
        ],
        axis=0,
    )
    (
        first_up_gradient,
        first_down_gradient,
        attention_in_gradient,
        attention_out_gradient,
        pointwise_in_gradient,
        pointwise_out_gradient,
        second_up_gradient,
        second_down_gradient,
        quantizer_in_gradient,
        codebook_gradient,
        small_gradients,
    ) = gradients(
        (
            first_up_pair,
            first_down_pair,
            attention_in_pair,
            attention_out_pair,
            pointwise_in_pair,
            pointwise_out_pair,
            second_up_pair,
            second_down_pair,
            (quantizer_entry, adjoint_logits),
            (chances_low, adjoint_codes),
        ),
        jnp.pad(small_sums, ((0, padding), (0, 0))),
    )
    small_gradient = jnp.sum(small_gradients, axis=0) / float(lax.axis_size("wide"))
    norm_gains_gradient = small_gradient[:gain_rows]
    depthwise_kernel_gradient = small_gradient[gain_rows : gain_rows + taps]
    batch_affine_gradient = small_gradient[gain_rows + taps : small_rows]
    return (
        output,
        codes,
        frames_gradient,
        first_up_gradient,
        first_down_gradient,
        attention_in_gradient,
        attention_out_gradient,
        pointwise_in_gradient,
        pointwise_out_gradient,
        second_up_gradient,
        second_down_gradient,
        quantizer_in_gradient,
        codebook_gradient,
        norm_gains_gradient,
        depthwise_kernel_gradient,
        batch_affine_gradient,
    )


def solution(mesh):
    in_specs = (
        P(("wide", "narrow"), None),
        P(("wide", "narrow"), None),
        P(("wide", "narrow"), None),
        P(),
        P(("wide", "narrow"), None),
        P(("wide", "narrow"), None),
        P("narrow", None),
        P("narrow", None),
        P("narrow", None),
        P("narrow", None),
        P("narrow", None),
        P("narrow", None),
        P("narrow", None),
        P("narrow", None),
        P("narrow", None),
        P("narrow", None),
        P(None, "narrow"),
        P(None, "narrow"),
        P(None, "narrow"),
    )
    out_specs = (
        P(("wide", "narrow"), None),
        P(("wide", "narrow"), None),
        P(("wide", "narrow"), None),
        P("narrow", None),
        P("narrow", None),
        P("narrow", None),
        P("narrow", None),
        P("narrow", None),
        P("narrow", None),
        P("narrow", None),
        P("narrow", None),
        P("narrow", None),
        P("narrow", None),
        P(None, "narrow"),
        P(None, "narrow"),
        P(None, "narrow"),
    )
    return jax.shard_map(
        per_device, mesh=mesh, in_specs=in_specs, out_specs=out_specs, check_vma=False
    )
```
